512 devices in a mesh: grp: 2 (over y), blk: 128 (over z, x), uly: 2 (over core).
Axes of the slice: x: 4, y: 2, z: 32, core: 2. Of those that a mesh axis runs over, the one named last changes fastest.
The devices are a block of a 4x8x32 slice.
Arguments:
- query: bfloat16 [8192, 1152], P(('grp', 'blk', 'uly')), parts along dimension 0, may hold values from -6 to 6
- key: bfloat16 [8192, 1152], P(('grp', 'blk', 'uly')), parts along dimension 0, may hold values from -6 to 6
- value: bfloat16 [8192, 1152], P(('grp', 'blk', 'uly')), parts along dimension 0, may hold values from -6 to 6
- q_gain: float32 [96], replicated, may hold values from 1 to 2.5
- k_gain: float32 [96], replicated, may hold values from 1 to 2.5
- out_weight: bfloat16 [1152, 2304], P('uly'), may hold values from -0.1875 to 0.1875
Outputs:
- mixed: bfloat16 [8192, 2304], P(('grp', 'blk', 'uly')), parts along dimension 0
The draws below stay inside these ranges and needn't reach their ends.
There are 2 independent parts, one for each index of `grp`. The reference program is written for one: setup_inputs(seed, part) draws one part's arguments, and reference() takes and returns one part's arrays. A program takes and returns all parts, laid end to end along the dimension named above; an argument that names none is the same for every part. Nothing has to cross between parts.
All inputs are finite; a program needn't handle non-finite values.
Results may differ from the reference program's by a relative error of at most 0.012.
Values may be sent and summed in bfloat16 or wider, within the bound.
A program may use at most 128 MiB of HBM per device.

```python
import jax
import jax.numpy as jnp
from jax import lax

H = 12
HD = 96
D = 2304
S = 4096


def steps_of(stream_key, extent, pieces, least, top_value):
    def one(position, shards_of):
        heights = jax.random.uniform(jax.random.fold_in(jax.random.fold_in(stream_key, 6), position), (shards_of,), jnp.float32, least / len(pieces), top_value / len(pieces))
        return jnp.repeat(jnp.exp(heights), extent[position] // shards_of).reshape((-1,) + (1,) * (len(extent) - position - 1))

    level = one(*pieces[0])
    for cut in pieces[1:]:
        level = level * one(*cut)
    return level


def normal_values(rng, shape, spread, most, shards=(), dtype=jnp.bfloat16):
    loudness = steps_of(rng, shape, shards, -0.22, 0.18) if shards else 1.0
    drawn = jax.random.normal(rng, shape, jnp.float32) * spread * loudness
    return jnp.minimum(jnp.maximum(drawn, -most), most).astype(dtype)


def setup_inputs(seed: int = 0, part: int = 0) -> dict:
    seeds = jax.random.split(jax.random.key(seed), 7)
    part_splits = jax.random.split(jax.random.fold_in(seeds[6], part), 7)
    query = normal_values(part_splits[0], (S, H * HD), 1.0, 6.0, ((0, 256),))
    key = normal_values(part_splits[1], (S, H * HD), 1.0, 6.0, ((0, 256),))
    value = normal_values(part_splits[2], (S, H * HD), 1.0, 6.0, ((0, 256),))
    q_gain = jnp.clip(jax.random.uniform(seeds[3], (HD,), jnp.float32, 1.0, 2.5), 1.0, 2.5)
    k_gain = jnp.clip(jax.random.uniform(seeds[4], (HD,), jnp.float32, 1.0, 2.5), 1.0, 2.5)
    out_weight = normal_values(seeds[5], (H * HD, D), (H * HD) ** -0.5, 0.1875, ((0, 2),))
    return {"query": query, "key": key, "value": value, "q_gain": q_gain, "k_gain": k_gain, "out_weight": out_weight}


def normed(data, gain):
    count = data.shape[0]
    grid = data.astype(jnp.float32).reshape(count, H, HD)
    meansq = lax.optimization_barrier(jnp.mean(grid * grid, axis=-1, keepdims=True))
    return (grid * lax.rsqrt(meansq + 1e-06) * gain).astype(jnp.bfloat16)

def reference(query, key, value, q_gain, k_gain, out_weight):
    count = query.shape[0]
    query_heads = jnp.transpose(normed(query, q_gain), (1, 0, 2))
    key_heads = jnp.transpose(normed(key, k_gain), (1, 0, 2))
    value_heads = jnp.transpose(value.reshape(count, H, HD), (1, 0, 2))
    score_scale = float(HD) ** (-0.5)

    def one_head(operands):
        query_one, key_one, value_one = operands
        scores = jnp.dot(query_one, key_one.T, preferred_element_type=jnp.float32) * score_scale
        expd = jnp.exp(scores)
        total_weight = lax.optimization_barrier(jnp.sum(expd, axis=1))
        weighted = jnp.dot(expd.astype(jnp.bfloat16), value_one, preferred_element_type=jnp.float32)
        return (weighted / total_weight[:, None]).astype(jnp.bfloat16)
    attn = lax.map(one_head, (query_heads, key_heads, value_heads))
    attn = jnp.transpose(attn, (1, 0, 2)).reshape(count, H * HD)
    return jnp.dot(attn, out_weight, preferred_element_type=jnp.float32).astype(jnp.bfloat16)
```

```python
import functools
import math

import jax
import jax.numpy as jnp
from jax import lax
from jax.experimental import pallas as pl
from jax.experimental.pallas import tpu as pltpu
from jax.sharding import PartitionSpec as P

HD = 96
PAD = 128
COLUMNS = 4
ROWS = 2
RING_CORE = 1
MESH = pl.DeviceIdType.MESH
TN = (((1,), (1,)), ((), ()))


def kernel(
    nodes,
    heads,
    query,
    key,
    value,
    q_gain,
    k_gain,
    weight,
    mixed,
    stage,
    key_raw,
    value_raw,
    query_raw,
    turned,
    gain_pad,
    own,
    opposite,
    ring,
    q_heads,
    totals,
    parts_out,
    parts_in,
    whole_weight,
    stage_sem,
    feed_send,
    feed_recv,
    ring_send,
    ring_recv,
    far_send,
    far_recv,
    back_send,
    back_recv,
    weight_sem,
):
    f32, bf16 = jnp.float32, jnp.bfloat16
    block = lax.axis_index("blk")
    core = lax.axis_index("uly")
    z, x = lax.div(block, COLUMNS), lax.rem(block, COLUMNS)
    z_block, z_row = lax.div(z, ROWS), lax.rem(z, ROWS)
    on_ring = core == RING_CORE
    tokens = query.shape[0]
    window = 3 * PAD
    lanes = 2 * PAD
    group = heads * HD
    line = 2 * COLUMNS * tokens
    half = nodes // 2
    pieces = 2 * heads

    def device(row, column, a_core):
        return {"blk": row * COLUMNS + column, "uly": a_core}

    def other_row(r):
        return z_block * ROWS + lax.rem(z_row + r, ROWS)

    def other_column(d):
        return lax.rem(x + d, COLUMNS)

    ahead = lax.rem(z + ROWS, nodes * ROWS)
    behind = lax.rem(z + (nodes - 1) * ROWS, nodes * ROWS)

    staged = [
        pltpu.make_async_copy(src, stage.at[i], stage_sem.at[i])
        for i, src in enumerate((key, value, query))
    ]
    for copy in staged:
        copy.start()

    barrier = pltpu.get_barrier_semaphore()

    def greet(dev):
        pl.semaphore_signal(barrier, inc=1, device_id=dev, device_id_type=MESH)

    for r in range(ROWS):
        for d in range(COLUMNS):
            if (r, d) != (0, 0):
                greet(device(other_row(r), other_column(d), RING_CORE))
    greet(device(z, x, 1 - core))

    @pl.when(on_ring)
    def _():
        for r in range(ROWS):
            for d in range(COLUMNS):
                if (r, d) != (0, 0):
                    greet(device(other_row(r), other_column(d), 1 - RING_CORE))
        greet(device(ahead, x, RING_CORE))
        greet(device(behind, x, RING_CORE))
        pl.semaphore_wait(barrier, 2 * ROWS * COLUMNS - 1 + 2)

    @pl.when(core != RING_CORE)
    def _():
        pl.semaphore_wait(barrier, ROWS * COLUMNS)

    place = pl.ds(pl.multiple_of((x * 2 + core) * tokens, tokens), tokens)

    def feed(i, r, d):
        column = other_column(d)
        dst = (key_raw, value_raw, query_raw.at[z_row])[i].at[place]
        recv = feed_recv.at[i] if i < 2 else feed_recv.at[2 + z_row]
        return pltpu.make_async_remote_copy(
            src_ref=stage.at[i, :, pl.ds(pl.multiple_of(column * lanes, PAD), window)],
            dst_ref=dst,
            send_sem=feed_send.at[i * COLUMNS + d if i < 2 else (2 + r) * COLUMNS + d],
            recv_sem=recv,
            device_id=device(other_row(r), column, RING_CORE),
            device_id_type=MESH,
        )

    def own_feed(i):
        dst = (key_raw, value_raw, query_raw.at[z_row])[i].at[place]
        recv = feed_recv.at[i] if i < 2 else feed_recv.at[2 + z_row]
        src = (key, value, query)[i]
        return pltpu.make_async_copy(
            src.at[:, pl.ds(pl.multiple_of(x * lanes, PAD), window)], dst, recv
        )

    feeds = [(i, r, d) for i in range(3) for r in range(ROWS if i == 2 else 1) for d in (2, 1, 3, 0)]
    for i, r, d in feeds:
        if (r, d) == (0, 2):
            staged[i].wait()
        if (r, d) == (0, 0):

            @pl.when(on_ring)
            def _():
                own_feed(i).start()

            @pl.when(core != RING_CORE)
            def _():
                feed(i, r, d).start()

        else:
            feed(i, r, d).start()

    depth = weight.shape[0]
    mine = whole_weight.at[pl.ds(pl.multiple_of(core * depth, 16), depth)]
    local_weight = pltpu.make_async_copy(weight, mine, weight_sem.at[0])
    sent_weight = pltpu.make_async_remote_copy(
        src_ref=weight,
        dst_ref=mine,
        send_sem=weight_sem.at[1],
        recv_sem=weight_sem.at[2],
        device_id=device(z, x, 1 - core),
        device_id_type=MESH,
    )
    local_weight.start()
    sent_weight.start()

    def give_back(r, d, c):
        column, a_core = other_column(d), lax.rem(core + c, 2)
        row = lax.rem(z_row + r, ROWS)
        start = row * line + (column * 2 + a_core) * tokens
        return pltpu.make_async_remote_copy(
            src_ref=parts_out.at[pl.ds(pl.multiple_of(start, tokens), tokens)],
            dst_ref=parts_in.at[z_row, x],
            send_sem=back_send.at[(r * COLUMNS + d) * 2 + c],
            recv_sem=back_recv.at[z_row * COLUMNS + x],
            device_id=device(other_row(r), column, a_core),
            device_id_type=MESH,
        )

    backs = [(r, d, c) for r in range(ROWS) for d in range(COLUMNS) for c in range(2)]

    @pl.when(on_ring)
    def _():
        for i, gain in enumerate((q_gain, k_gain)):
            gain_pad[...] = jnp.zeros_like(gain_pad)
            gain_pad[:, 0:HD] = jnp.broadcast_to(gain[...], (PAD, HD))
            turned[i, 0:PAD, :] = gain_pad[...].T
        q_column, k_column = turned[0, 0:HD, :], turned[1, 0:HD, :]
        first = x * (group - lanes)

        def head_of(i, h):
            return turned[i, pl.ds(pl.multiple_of(first + h * HD, 32), HD), :]

        def normed(data, gain):
            meansq = jnp.mean(data * data, axis=0, keepdims=True)
            return data * lax.rsqrt(meansq + 1e-06) * gain

        pltpu.make_async_copy(key_raw, key_raw, feed_recv.at[0]).wait()
        turned[0] = key_raw[...].astype(f32).T
        for h in range(heads):
            own[2 * h] = normed(head_of(0, h), k_column).astype(bf16)
        pltpu.make_async_copy(value_raw, value_raw, feed_recv.at[1]).wait()
        turned[1] = value_raw[...].astype(f32).T
        for h in range(heads):
            own[2 * h + 1] = head_of(1, h).astype(bf16)

        def to(way, slot, p, src, step):
            if isinstance(step, int) and step == half - 1:
                dst, send, recv = opposite.at[p], far_send.at[p], far_recv.at[p]
            else:
                dst, send, recv = ring.at[way, step, p], ring_send.at[way, step, p], ring_recv.at[way, step, p]
            return pltpu.make_async_remote_copy(
                src_ref=src,
                dst_ref=dst,
                send_sem=send,
                recv_sem=recv,
                device_id=device(ahead if way == 0 else behind, x, RING_CORE),
                device_id_type=MESH,
            )

        for p in range(pieces):
            for way in range(2):
                to(way, 0, p, own.at[p], 0).start()

        for r in range(ROWS):
            rows = query_raw.at[r]
            pltpu.make_async_copy(rows, rows, feed_recv.at[2 + r]).wait()
            turned[0] = query_raw[r].astype(f32).T
            for h in range(heads):
                data = normed(head_of(0, h), q_column)
                data = jnp.concatenate([data, jnp.zeros((PAD - HD, line), f32)], axis=0)
                q_heads[h, r * line : (r + 1) * line, :] = data.T.astype(bf16)

        scale = float(HD) ** (-0.5) * math.log2(math.e)

        def attend(h, keys, values, fresh=False):
            wide = line * len(keys)
            k = jnp.concatenate(
                [jnp.concatenate(keys, axis=1), jnp.zeros((PAD - HD, wide), bf16)], axis=0
            )
            v = jnp.concatenate(
                [jnp.concatenate(values, axis=1), jnp.ones((PAD - HD, wide), bf16)], axis=0
            )
            scores = jnp.dot(q_heads[h], k, preferred_element_type=f32)
            expd = jnp.exp2(scores * scale).astype(bf16)
            total = lax.dot_general(expd, v, TN, preferred_element_type=f32)
            if fresh:
                totals[h] = total
            else:
                totals[h] += total

        for h in range(heads):
            attend(h, [own[2 * h]], [own[2 * h + 1]], True)

        def ring_step(step, last):
            for h in range(heads):
                for p in (2 * h, 2 * h + 1):
                    for way in range(2):
                        to(way, 0, p, own.at[p], step).wait_recv()
                        if not last:
                            to(way, 0, p, ring.at[way, step, p], step + 1).start()
                        elif (p < pieces // 2) == (way == 0):
                            to(way, 0, p, ring.at[way, step, p], half - 1).start()
                attend(
                    h,
                    [ring[0, step, 2 * h], ring[1, step, 2 * h]],
                    [ring[0, step, 2 * h + 1], ring[1, step, 2 * h + 1]],
                )

        def body(step, carry):
            ring_step(step, False)
            return carry

        lax.fori_loop(0, half - 2, body, 0)
        ring_step(half - 2, True)

        lane = lax.broadcasted_iota(jnp.int32, (ROWS * line, PAD), 1)
        for h in range(heads):
            for p in (2 * h, 2 * h + 1):
                way = 0 if p < pieces // 2 else 1
                to(way, 0, p, own.at[p], half - 1).wait_recv()
            attend(h, [opposite[2 * h]], [opposite[2 * h + 1]])
            total = totals[h]
            high = total.astype(bf16)
            low = (total - high.astype(f32)).astype(bf16)
            parts_out[:, h * PAD : (h + 1) * PAD] = jnp.where(lane >= HD + 16, low, high)

        for r, d, c in backs:
            if (r, d, c) != (0, 0, 0):
                give_back(r, d, c).start()
        own_start = z_row * line + (x * 2 + core) * tokens
        parts_in[z_row, x] = parts_out[pl.ds(pl.multiple_of(own_start, tokens), tokens)]

    local_weight.wait()
    sent_weight.wait()
    attn = []
    for i in range(ROWS * COLUMNS):
        r, d = i // COLUMNS, i % COLUMNS
        itself = (z_row == r) & (x == d) & on_ring

        @pl.when(jnp.logical_not(itself))
        def _():
            pltpu.make_async_copy(parts_in.at[r, d], parts_in.at[r, d], back_recv.at[i]).wait()

    for d in range(COLUMNS):
        for h in range(heads):
            part = sum(
                parts_in[r, d, :, h * PAD : (h + 1) * PAD].astype(f32) for r in range(ROWS)
            )
            total_weight = part[:, HD : HD + 1] + part[:, HD + 16 : HD + 17]
            attn.append((part[:, 0:HD] / total_weight).astype(bf16))
    attn = jnp.concatenate(attn, axis=1)
    mixed[...] = jnp.dot(attn, whole_weight[...], preferred_element_type=f32).astype(bf16)

    for i, r, d in feeds:
        if (r, d) == (0, 0):

            @pl.when(core != RING_CORE)
            def _():
                feed(i, r, d).wait_send()

        else:
            feed(i, r, d).wait_send()

    @pl.when(on_ring)
    def _():
        def sent(step, carry):
            for way in range(2):
                for p in range(pieces):
                    pltpu.make_async_copy(
                        ring.at[way, step, p], ring.at[way, step, p], ring_send.at[way, step, p]
                    ).wait()
            return carry

        lax.fori_loop(0, half - 1, sent, 0)
        for p in range(pieces):
            pltpu.make_async_copy(opposite.at[p], opposite.at[p], far_send.at[p]).wait()
        for r, d, c in backs:
            if (r, d, c) != (0, 0, 0):
                give_back(r, d, c).wait_send()


def on_device(lines, query, key, value, q_gain, k_gain, out_weight):
    tokens, width = query.shape
    heads = width // HD // COLUMNS
    nodes = lines // ROWS
    half = nodes // 2
    pieces = 2 * heads
    line = 2 * COLUMNS * tokens
    window = 3 * PAD
    f32, bf16 = jnp.float32, jnp.bfloat16
    hbm = pl.BlockSpec(memory_space=pl.ANY)
    vmem = pl.BlockSpec(memory_space=pltpu.VMEM)
    dma = pltpu.SemaphoreType.DMA
    return pl.pallas_call(
        functools.partial(kernel, nodes, heads),
        out_shape=jax.ShapeDtypeStruct((tokens, out_weight.shape[1]), bf16),
        in_specs=[hbm, hbm, hbm, vmem, vmem, hbm],
        out_specs=vmem,
        scratch_shapes=[
            pltpu.VMEM((3, tokens, width), bf16),
            pltpu.VMEM((line, window), bf16),
            pltpu.VMEM((line, window), bf16),
            pltpu.VMEM((ROWS, line, window), bf16),
            pltpu.VMEM((2, window, line), f32),
            pltpu.VMEM((PAD, PAD), f32),
            pltpu.VMEM((pieces, HD, line), bf16),
            pltpu.VMEM((pieces, HD, line), bf16),
            pltpu.VMEM((2, half - 1, pieces, HD, line), bf16),
            pltpu.VMEM((heads, ROWS * line, PAD), bf16),
            pltpu.VMEM((heads, ROWS * line, PAD), f32),
            pltpu.VMEM((ROWS * line, heads * PAD), bf16),
            pltpu.VMEM((ROWS, COLUMNS, tokens, heads * PAD), bf16),
            pltpu.VMEM((2 * out_weight.shape[0], out_weight.shape[1]), bf16),
            dma((3,)),
            dma(((2 + ROWS) * COLUMNS,)),
            dma((2 + ROWS,)),
            dma((2, half - 1, pieces)),
            dma((2, half - 1, pieces)),
            dma((pieces,)),
            dma((pieces,)),
            dma((ROWS * COLUMNS * 2,)),
            dma((ROWS * COLUMNS,)),
            dma((3,)),
        ],
        compiler_params=pltpu.CompilerParams(collective_id=0, has_side_effects=True),
        name="attention",
    )(query, key, value, q_gain.reshape(1, HD), k_gain.reshape(1, HD), out_weight)


def solution(mesh):
    tokens = P(("grp", "blk", "uly"), None)
    return jax.shard_map(
        functools.partial(on_device, mesh.shape["blk"] // COLUMNS),
        mesh=mesh,
        in_specs=(tokens, tokens, tokens, P(), P(), P("uly", None)),
        out_specs=tokens,
        check_vma=False,
    )
```

```python
import functools
import math

import jax
import jax.numpy as jnp
from jax import lax
from jax.experimental import pallas as pl
from jax.experimental.pallas import tpu as pltpu
from jax.sharding import PartitionSpec as P

HD = 96
PAD = 128
COLUMNS = 4
ROWS = 2
RING_CORE = 1
AHEAD = 6
MESH = pl.DeviceIdType.MESH
TN = (((1,), (1,)), ((), ()))


def kernel(
    nodes,
    heads,
    query,
    key,
    value,
    q_gain,
    k_gain,
    weight,
    mixed,
    stage,
    key_raw,
    value_raw,
    query_raw,
    turned,
    gain_pad,
    own,
    ring,
    q_heads,
    totals,
    parts_out,
    parts_in,
    whole_weight,
    stage_sem,
    feed_send,
    feed_recv,
    ring_send,
    ring_recv,
    back_send,
    back_recv,
    weight_sem,
    ready,
):
    f32, bf16 = jnp.float32, jnp.bfloat16
    block = lax.axis_index("blk")
    core = lax.axis_index("uly")
    z, x = lax.div(block, COLUMNS), lax.rem(block, COLUMNS)
    z_block, z_row = lax.div(z, ROWS), lax.rem(z, ROWS)
    on_ring = core == RING_CORE
    tokens = query.shape[0]
    window = 3 * PAD
    lanes = 2 * PAD
    group = heads * HD
    line = 2 * COLUMNS * tokens
    pieces = 2 * heads
    most = (AHEAD, nodes - 1 - AHEAD)

    def device(row, column, a_core):
        return {"blk": row * COLUMNS + column, "uly": a_core}

    def other_row(r):
        return z_block * ROWS + lax.rem(z_row + r, ROWS)

    def other_column(d):
        return lax.rem(x + d, COLUMNS)

    node, last_node = z_block, nodes - 1
    ahead = lax.rem(z + ROWS, nodes * ROWS)
    behind = lax.rem(z + last_node * ROWS, nodes * ROWS)
    is_first, is_last = node == 0, node == last_node

    staged = [
        pltpu.make_async_copy(src, stage.at[i], stage_sem.at[i])
        for i, src in enumerate((key, value, query))
    ]
    for copy in staged:
        copy.start()

    barrier = pltpu.get_barrier_semaphore()

    def greet(dev):
        pl.semaphore_signal(barrier, inc=1, device_id=dev, device_id_type=MESH)

    for r in range(ROWS):
        for d in range(COLUMNS):
            if (r, d) != (0, 0):
                greet(device(other_row(r), other_column(d), RING_CORE))
    greet(device(z, x, 1 - core))

    @pl.when(on_ring)
    def _():
        for r in range(ROWS):
            for d in range(COLUMNS):
                if (r, d) != (0, 0):
                    greet(device(other_row(r), other_column(d), 1 - RING_CORE))

        @pl.when(jnp.logical_not(is_last))
        def _():
            greet(device(ahead, x, RING_CORE))

        @pl.when(is_first)
        def _():
            greet(device(behind, x, RING_CORE))

        lower = jnp.where(is_first, 0, 1) + jnp.where(is_last, 1, 0)
        pl.semaphore_wait(barrier, 2 * ROWS * COLUMNS - 1 + lower)

        @pl.when(jnp.logical_not(is_first))
        def _():
            pl.semaphore_signal(
                ready.at[0], inc=1, device_id=device(behind, x, RING_CORE), device_id_type=MESH
            )

        @pl.when(is_last)
        def _():
            pl.semaphore_signal(
                ready.at[1], inc=1, device_id=device(ahead, x, RING_CORE), device_id_type=MESH
            )

    @pl.when(core != RING_CORE)
    def _():
        pl.semaphore_wait(barrier, ROWS * COLUMNS)

    place = pl.ds(pl.multiple_of((x * 2 + core) * tokens, tokens), tokens)

    def feed(i, r, d):
        column = other_column(d)
        dst = (key_raw, value_raw, query_raw.at[z_row])[i].at[place]
        recv = feed_recv.at[i] if i < 2 else feed_recv.at[2 + z_row]
        return pltpu.make_async_remote_copy(
            src_ref=stage.at[i, :, pl.ds(pl.multiple_of(column * lanes, PAD), window)],
            dst_ref=dst,
            send_sem=feed_send.at[i * COLUMNS + d if i < 2 else (2 + r) * COLUMNS + d],
            recv_sem=recv,
            device_id=device(other_row(r), column, RING_CORE),
            device_id_type=MESH,
        )

    def own_feed(i):
        dst = (key_raw, value_raw, query_raw.at[z_row])[i].at[place]
        recv = feed_recv.at[i] if i < 2 else feed_recv.at[2 + z_row]
        src = (key, value, query)[i]
        return pltpu.make_async_copy(
            src.at[:, pl.ds(pl.multiple_of(x * lanes, PAD), window)], dst, recv
        )

    feeds = [(i, r, d) for i in range(3) for r in range(ROWS if i == 2 else 1) for d in (2, 1, 3, 0)]
    for i, r, d in feeds:
        if (r, d) == (0, 2):
            staged[i].wait()
        if (r, d) == (0, 0):

            @pl.when(on_ring)
            def _():
                own_feed(i).start()

            @pl.when(core != RING_CORE)
            def _():
                feed(i, r, d).start()

        else:
            feed(i, r, d).start()

    depth = weight.shape[0]
    mine = whole_weight.at[pl.ds(pl.multiple_of(core * depth, 16), depth)]
    local_weight = pltpu.make_async_copy(weight, mine, weight_sem.at[0])
    sent_weight = pltpu.make_async_remote_copy(
        src_ref=weight,
        dst_ref=mine,
        send_sem=weight_sem.at[1],
        recv_sem=weight_sem.at[2],
        device_id=device(z, x, 1 - core),
        device_id_type=MESH,
    )
    local_weight.start()
    sent_weight.start()

    def give_back(r, d, c):
        column, a_core = other_column(d), lax.rem(core + c, 2)
        row = lax.rem(z_row + r, ROWS)
        start = row * line + (column * 2 + a_core) * tokens
        return pltpu.make_async_remote_copy(
            src_ref=parts_out.at[pl.ds(pl.multiple_of(start, tokens), tokens)],
            dst_ref=parts_in.at[z_row, x],
            send_sem=back_send.at[(r * COLUMNS + d) * 2 + c],
            recv_sem=back_recv.at[z_row * COLUMNS + x],
            device_id=device(other_row(r), column, a_core),
            device_id_type=MESH,
        )

    backs = [(r, d, c) for r in range(ROWS) for d in range(COLUMNS) for c in range(2)]

    @pl.when(on_ring)
    def _():
        for i, gain in enumerate((q_gain, k_gain)):
            gain_pad[...] = jnp.zeros_like(gain_pad)
            gain_pad[:, 0:HD] = jnp.broadcast_to(gain[...], (PAD, HD))
            turned[i, 0:PAD, :] = gain_pad[...].T
        q_column, k_column = turned[0, 0:HD, :], turned[1, 0:HD, :]
        first = x * (group - lanes)

        def head_of(i, h):
            return turned[i, pl.ds(pl.multiple_of(first + h * HD, 32), HD), :]

        def normed(data, gain):
            meansq = jnp.mean(data * data, axis=0, keepdims=True)
            return data * lax.rsqrt(meansq + 1e-06) * gain

        pltpu.make_async_copy(key_raw, key_raw, feed_recv.at[0]).wait()
        turned[0] = key_raw[...].astype(f32).T
        for h in range(heads):
            own[2 * h] = normed(head_of(0, h), k_column).astype(bf16)
        pltpu.make_async_copy(value_raw, value_raw, feed_recv.at[1]).wait()
        turned[1] = value_raw[...].astype(f32).T
        for h in range(heads):
            own[2 * h + 1] = head_of(1, h).astype(bf16)

        def landing(way, step, p, src):
            return pltpu.make_async_remote_copy(
                src_ref=src,
                dst_ref=ring.at[way, step, p],
                send_sem=ring_send.at[way, step, p],
                recv_sem=ring_recv.at[way, step, p],
                device_id=device(jnp.where(way == 0, ahead, behind), x, RING_CORE),
                device_id_type=MESH,
            )

        def send_own(way):
            for p in range(pieces):
                landing(way, 0, p, own.at[p]).start()

        @pl.when(jnp.logical_not(is_last))
        def _():
            pl.semaphore_wait(ready.at[0], 1)

        send_own(0)

        @pl.when(jnp.logical_not(is_first))
        def _():
            send_own(1)

        for r in range(ROWS):
            rows = query_raw.at[r]
            pltpu.make_async_copy(rows, rows, feed_recv.at[2 + r]).wait()
            turned[0] = query_raw[r].astype(f32).T
            for h in range(heads):
                data = normed(head_of(0, h), q_column)
                data = jnp.concatenate([data, jnp.zeros((PAD - HD, line), f32)], axis=0)
                q_heads[h, r * line : (r + 1) * line, :] = data.T.astype(bf16)

        scale = float(HD) ** (-0.5) * math.log2(math.e)

        def attend(h, keys, values, fresh=False):
            wide = line * len(keys)
            k = jnp.concatenate(
                [jnp.concatenate(keys, axis=1), jnp.zeros((PAD - HD, wide), bf16)], axis=0
            )
            v = jnp.concatenate(
                [jnp.concatenate(values, axis=1), jnp.ones((PAD - HD, wide), bf16)], axis=0
            )
            scores = jnp.dot(q_heads[h], k, preferred_element_type=f32)
            expd = jnp.exp2(scores * scale).astype(bf16)
            total = lax.dot_general(expd, v, TN, preferred_element_type=f32)
            if fresh:
                totals[h] = total
            else:
                totals[h] += total

        for h in range(heads):
            attend(h, [own[2 * h]], [own[2 * h + 1]], True)

        def opens(m):
            return jnp.minimum(40 * m, 160 + 20 * m)

        def from_behind(step):
            m = node - 1 - step
            return jnp.where(
                m >= 0, opens(node) + 15 * step, opens(m + nodes) + 50 + 26 * (step + 1)
            )

        def from_ahead(step):
            m = node + 1 + step
            return jnp.where(
                m < nodes,
                opens(m) + 50 + 26 * (step + 1),
                opens(last_node) + 80 + 26 * (last_node - node) + 16 * (m - nodes + 1),
            )

        def chunk(t, steps):
            up, down = steps
            take_up = (down >= most[1]) | ((up < most[0]) & (from_behind(up) <= from_ahead(down)))

            @pl.when(is_first & take_up & (up == 0))
            def _():
                pl.semaphore_wait(ready.at[1], 1)
                send_own(1)

                def held(step, carry):
                    for p in range(pieces):
                        landing(1, step + 1, p, ring.at[1, step, p]).start()
                    return carry

                lax.fori_loop(0, jnp.minimum(down, most[1] - 1), held, 0)

            way = jnp.where(take_up, 0, 1)
            step = jnp.where(take_up, up, down)
            passes = jnp.where(take_up, up < most[0] - 1, (down < most[1] - 1) & ~(is_first & (up == 0)))
            for h in range(heads):
                for p in (2 * h, 2 * h + 1):
                    landing(way, step, p, own.at[p]).wait_recv()

                    @pl.when(passes)
                    def _():
                        landing(way, step + 1, p, ring.at[way, step, p]).start()

                attend(h, [ring[way, step, 2 * h]], [ring[way, step, 2 * h + 1]])
            return (jnp.where(take_up, up + 1, up), jnp.where(take_up, down, down + 1))

        lax.fori_loop(0, nodes - 1, chunk, (jnp.int32(0), jnp.int32(0)))

        lane = lax.broadcasted_iota(jnp.int32, (ROWS * line, PAD), 1)
        for h in range(heads):
            total = totals[h]
            high = total.astype(bf16)
            low = (total - high.astype(f32)).astype(bf16)
            parts_out[:, h * PAD : (h + 1) * PAD] = jnp.where(lane >= HD + 16, low, high)

        for r, d, c in backs:
            if (r, d, c) != (0, 0, 0):
                give_back(r, d, c).start()
        own_start = z_row * line + (x * 2 + core) * tokens
        parts_in[z_row, x] = parts_out[pl.ds(pl.multiple_of(own_start, tokens), tokens)]

    local_weight.wait()
    sent_weight.wait()
    attn = []
    for i in range(ROWS * COLUMNS):
        r, d = i // COLUMNS, i % COLUMNS
        itself = (z_row == r) & (x == d) & on_ring

        @pl.when(jnp.logical_not(itself))
        def _():
            pltpu.make_async_copy(parts_in.at[r, d], parts_in.at[r, d], back_recv.at[i]).wait()

    for d in range(COLUMNS):
        for h in range(heads):
            part = sum(
                parts_in[r, d, :, h * PAD : (h + 1) * PAD].astype(f32) for r in range(ROWS)
            )
            total_weight = part[:, HD : HD + 1] + part[:, HD + 16 : HD + 17]
            attn.append((part[:, 0:HD] / total_weight).astype(bf16))
    attn = jnp.concatenate(attn, axis=1)
    mixed[...] = jnp.dot(attn, whole_weight[...], preferred_element_type=f32).astype(bf16)

    for i, r, d in feeds:
        if (r, d) == (0, 0):

            @pl.when(core != RING_CORE)
            def _():
                feed(i, r, d).wait_send()

        else:
            feed(i, r, d).wait_send()

    @pl.when(on_ring)
    def _():
        for way in range(2):

            def sent(step, carry):
                for p in range(pieces):
                    pltpu.make_async_copy(
                        ring.at[way, step, p], ring.at[way, step, p], ring_send.at[way, step, p]
                    ).wait()
                return carry

            lax.fori_loop(0, most[way], sent, 0)
        for r, d, c in backs:
            if (r, d, c) != (0, 0, 0):
                give_back(r, d, c).wait_send()


def on_device(lines, query, key, value, q_gain, k_gain, out_weight):
    tokens, width = query.shape
    heads = width // HD // COLUMNS
    nodes = lines // ROWS
    pieces = 2 * heads
    most = max(AHEAD, nodes - 1 - AHEAD)
    line = 2 * COLUMNS * tokens
    window = 3 * PAD
    f32, bf16 = jnp.float32, jnp.bfloat16
    hbm = pl.BlockSpec(memory_space=pl.ANY)
    vmem = pl.BlockSpec(memory_space=pltpu.VMEM)
    dma = pltpu.SemaphoreType.DMA
    return pl.pallas_call(
        functools.partial(kernel, nodes, heads),
        out_shape=jax.ShapeDtypeStruct((tokens, out_weight.shape[1]), bf16),
        in_specs=[hbm, hbm, hbm, vmem, vmem, hbm],
        out_specs=vmem,
        scratch_shapes=[
            pltpu.VMEM((3, tokens, width), bf16),
            pltpu.VMEM((line, window), bf16),
            pltpu.VMEM((line, window), bf16),
            pltpu.VMEM((ROWS, line, window), bf16),
            pltpu.VMEM((2, window, line), f32),
            pltpu.VMEM((PAD, PAD), f32),
            pltpu.VMEM((pieces, HD, line), bf16),
            pltpu.VMEM((2, most, pieces, HD, line), bf16),
            pltpu.VMEM((heads, ROWS * line, PAD), bf16),
            pltpu.VMEM((heads, ROWS * line, PAD), f32),
            pltpu.VMEM((ROWS * line, heads * PAD), bf16),
            pltpu.VMEM((ROWS, COLUMNS, tokens, heads * PAD), bf16),
            pltpu.VMEM((2 * out_weight.shape[0], out_weight.shape[1]), bf16),
            dma((3,)),
            dma(((2 + ROWS) * COLUMNS,)),
            dma((2 + ROWS,)),
            dma((2, most, pieces)),
            dma((2, most, pieces)),
            dma((ROWS * COLUMNS * 2,)),
            dma((ROWS * COLUMNS,)),
            dma((3,)),
            pltpu.SemaphoreType.REGULAR((2,)),
        ],
        compiler_params=pltpu.CompilerParams(collective_id=0, has_side_effects=True),
        name="attention",
    )(query, key, value, q_gain.reshape(1, HD), k_gain.reshape(1, HD), out_weight)


def solution(mesh):
    tokens = P(("grp", "blk", "uly"), None)
    return jax.shard_map(
        functools.partial(on_device, mesh.shape["blk"] // COLUMNS),
        mesh=mesh,
        in_specs=(tokens, tokens, tokens, P(), P(), P("uly", None)),
        out_specs=tokens,
        check_vma=False,
    )
```

```python
import functools
import math

import jax
import jax.numpy as jnp
from jax import lax
from jax.experimental import pallas as pl
from jax.experimental.pallas import tpu as pltpu
from jax.sharding import PartitionSpec as P

HD = 96
PAD = 128
COLUMNS = 4
ROWS = 2
FEED_CORE = 1
AHEAD = 6
MESH = pl.DeviceIdType.MESH
TN = (((1,), (1,)), ((), ()))


def kernel(
    nodes,
    heads,
    query,
    key,
    value,
    q_gain,
    k_gain,
    weight,
    mixed,
    stage,
    key_raw,
    value_raw,
    query_raw,
    turned,
    gain_pad,
    own,
    ring,
    q_heads,
    totals,
    parts_out,
    parts_in,
    whole_weight,
    stage_sem,
    feed_send,
    feed_recv,
    ring_send,
    ring_recv,
    back_send,
    back_recv,
    weight_sem,
    pair_send,
    pair_recv,
    ready,
):
    f32, bf16 = jnp.float32, jnp.bfloat16
    block = lax.axis_index("blk")
    core = lax.axis_index("uly")
    z, x = lax.div(block, COLUMNS), lax.rem(block, COLUMNS)
    z_block, z_row = lax.div(z, ROWS), lax.rem(z, ROWS)
    feeds_pair = core == FEED_CORE
    tokens = query.shape[0]
    window = 3 * PAD
    lanes = 2 * PAD
    group = heads * HD
    line = 2 * COLUMNS * tokens
    pieces = 2 * heads
    steps = jnp.where(feeds_pair, nodes - 1 - AHEAD, AHEAD)

    def device(row, column, a_core):
        return {"blk": row * COLUMNS + column, "uly": a_core}

    def other_row(r):
        return z_block * ROWS + lax.rem(z_row + r, ROWS)

    def other_column(d):
        return lax.rem(x + d, COLUMNS)

    node, last_node = z_block, nodes - 1
    ahead = lax.rem(z + ROWS, nodes * ROWS)
    behind = lax.rem(z + last_node * ROWS, nodes * ROWS)
    is_first, is_last = node == 0, node == last_node

    staged = [
        pltpu.make_async_copy(src, stage.at[i], stage_sem.at[i])
        for i, src in enumerate((key, value, query))
    ]
    for copy in staged:
        copy.start()

    barrier = pltpu.get_barrier_semaphore()

    def greet(dev):
        pl.semaphore_signal(barrier, inc=1, device_id=dev, device_id_type=MESH)

    for r in range(ROWS):
        for d in range(COLUMNS):
            for c in range(2):
                if (r, d, c) != (0, 0, 0):
                    greet(device(other_row(r), other_column(d), lax.rem(core + c, 2)))

    @pl.when(jnp.logical_not(is_last))
    def _():
        greet(device(ahead, x, core))

    @pl.when(is_first)
    def _():
        greet(device(behind, x, core))

    lower = jnp.where(is_first, 0, 1) + jnp.where(is_last, 1, 0)
    pl.semaphore_wait(barrier, 2 * ROWS * COLUMNS - 1 + lower)

    target = jnp.where(feeds_pair, behind, ahead)
    source = jnp.where(feeds_pair, ahead, behind)

    @pl.when(jnp.where(feeds_pair, node == last_node, node != 0))
    def _():
        pl.semaphore_signal(ready, inc=1, device_id=device(source, x, core), device_id_type=MESH)

    def wait_for_target():
        @pl.when(jnp.where(feeds_pair, node == 0, node != last_node))
        def _():
            pl.semaphore_wait(ready, 1)

    place = pl.ds(pl.multiple_of((x * 2 + core) * tokens, tokens), tokens)

    def feed(i, r, d):
        column = other_column(d)
        dst = (key_raw, value_raw, query_raw.at[z_row])[i].at[place]
        recv = feed_recv.at[i] if i < 2 else feed_recv.at[2 + z_row]
        return pltpu.make_async_remote_copy(
            src_ref=stage.at[i, :, pl.ds(pl.multiple_of(column * lanes, PAD), window)],
            dst_ref=dst,
            send_sem=feed_send.at[i * COLUMNS + d if i < 2 else (2 + r) * COLUMNS + d],
            recv_sem=recv,
            device_id=device(other_row(r), column, FEED_CORE),
            device_id_type=MESH,
        )

    def own_feed(i):
        dst = (key_raw, value_raw, query_raw.at[z_row])[i].at[place]
        recv = feed_recv.at[i] if i < 2 else feed_recv.at[2 + z_row]
        src = (key, value, query)[i]
        return pltpu.make_async_copy(
            src.at[:, pl.ds(pl.multiple_of(x * lanes, PAD), window)], dst, recv
        )

    feeds = [(i, r, d) for i in range(3) for r in range(ROWS if i == 2 else 1) for d in (2, 1, 3, 0)]
    for i, r, d in feeds:
        if (r, d) == (0, 2):
            staged[i].wait()
        if (r, d) == (0, 0):

            @pl.when(feeds_pair)
            def _():
                own_feed(i).start()

            @pl.when(core != FEED_CORE)
            def _():
                feed(i, r, d).start()

        else:
            feed(i, r, d).start()

    depth = weight.shape[0]
    mine = whole_weight.at[pl.ds(pl.multiple_of(core * depth, 16), depth)]
    local_weight = pltpu.make_async_copy(weight, mine, weight_sem.at[0])
    sent_weight = pltpu.make_async_remote_copy(
        src_ref=weight,
        dst_ref=mine,
        send_sem=weight_sem.at[1],
        recv_sem=weight_sem.at[2],
        device_id=device(z, x, 1 - core),
        device_id_type=MESH,
    )
    local_weight.start()
    sent_weight.start()

    def give_back(r, d, c):
        column, a_core = other_column(d), lax.rem(core + c, 2)
        row = lax.rem(z_row + r, ROWS)
        start = row * line + (column * 2 + a_core) * tokens
        return pltpu.make_async_remote_copy(
            src_ref=parts_out.at[pl.ds(pl.multiple_of(start, tokens), tokens)],
            dst_ref=parts_in.at[core, z_row, x],
            send_sem=back_send.at[(r * COLUMNS + d) * 2 + c],
            recv_sem=back_recv.at[(core * ROWS + z_row) * COLUMNS + x],
            device_id=device(other_row(r), column, a_core),
            device_id_type=MESH,
        )

    backs = [(r, d, c) for r in range(ROWS) for d in range(COLUMNS) for c in range(2)]

    def landing(step, p, src):
        return pltpu.make_async_remote_copy(
            src_ref=src,
            dst_ref=ring.at[step, p],
            send_sem=ring_send.at[step],
            recv_sem=ring_recv.at[step, p],
            device_id=device(target, x, core),
            device_id_type=MESH,
        )

    def to_pair(ref, p):
        return pltpu.make_async_remote_copy(
            src_ref=ref,
            dst_ref=ref,
            send_sem=pair_send.at[p],
            recv_sem=pair_recv.at[p],
            device_id=device(z, x, 1 - core),
            device_id_type=MESH,
        )

    scale = float(HD) ** (-0.5) * math.log2(math.e)

    def attend(h, k, v):
        k = jnp.concatenate([k, jnp.zeros((PAD - HD, line), bf16)], axis=0)
        v = jnp.concatenate([v, jnp.ones((PAD - HD, line), bf16)], axis=0)
        scores = jnp.dot(q_heads[h], k, preferred_element_type=f32)
        expd = jnp.exp2(scores * scale).astype(bf16)
        totals[h] += lax.dot_general(expd, v, TN, preferred_element_type=f32)

    totals[...] = jnp.zeros_like(totals)

    @pl.when(feeds_pair)
    def _():
        for i, gain in enumerate((q_gain, k_gain)):
            gain_pad[...] = jnp.zeros_like(gain_pad)
            gain_pad[:, 0:HD] = jnp.broadcast_to(gain[...], (PAD, HD))
            turned[i, 0:PAD, :] = gain_pad[...].T
        q_column, k_column = turned[0, 0:HD, :], turned[1, 0:HD, :]
        first = x * (group - lanes)

        def head_of(i, h):
            return turned[i, pl.ds(pl.multiple_of(first + h * HD, 32), HD), :]

        def normed(data, gain):
            meansq = jnp.mean(data * data, axis=0, keepdims=True)
            return data * lax.rsqrt(meansq + 1e-06) * gain

        pltpu.make_async_copy(key_raw, key_raw, feed_recv.at[0]).wait()
        turned[0] = key_raw[...].astype(f32).T
        for h in range(heads):
            own[2 * h] = normed(head_of(0, h), k_column).astype(bf16)
        pltpu.make_async_copy(value_raw, value_raw, feed_recv.at[1]).wait()
        turned[1] = value_raw[...].astype(f32).T
        for h in range(heads):
            own[2 * h + 1] = head_of(1, h).astype(bf16)

        @pl.when(node != 0)
        def _():
            for p in range(pieces):
                landing(0, p, own.at[p]).start()

        for p in range(pieces):
            to_pair(own.at[p], p).start()

        for r in range(ROWS):
            rows = query_raw.at[r]
            pltpu.make_async_copy(rows, rows, feed_recv.at[2 + r]).wait()
            turned[0] = query_raw[r].astype(f32).T
            for h in range(heads):
                data = normed(head_of(0, h), q_column)
                data = jnp.concatenate([data, jnp.zeros((PAD - HD, line), f32)], axis=0)
                q_heads[h, r * line : (r + 1) * line, :] = data.T.astype(bf16)

        for h in range(heads):
            to_pair(q_heads.at[h], pieces + h).start()
        for h in range(heads):
            attend(h, own[2 * h], own[2 * h + 1])
        wait_for_target()

        @pl.when(node == 0)
        def _():
            for p in range(pieces):
                landing(0, p, own.at[p]).start()

    @pl.when(core != FEED_CORE)
    def _():
        wait_for_target()
        for p in range(pieces):
            to_pair(own.at[p], p).wait_recv()
            landing(0, p, own.at[p]).start()
        for h in range(heads):
            to_pair(q_heads.at[h], pieces + h).wait_recv()

    def chunk(step, carry):
        for h in range(heads):
            for p in (2 * h, 2 * h + 1):
                landing(step, p, own.at[p]).wait_recv()

                @pl.when(step < steps - 1)
                def _():
                    landing(step + 1, p, ring.at[step, p]).start()

            attend(h, ring[step, 2 * h], ring[step, 2 * h + 1])
        return carry

    lax.fori_loop(0, steps, chunk, 0)

    lane = lax.broadcasted_iota(jnp.int32, (ROWS * line, PAD), 1)
    for h in range(heads):
        total = totals[h]
        high = total.astype(bf16)
        low = (total - high.astype(f32)).astype(bf16)
        parts_out[:, h * PAD : (h + 1) * PAD] = jnp.where(lane >= HD + 16, low, high)

    for r, d, c in backs:
        if (r, d, c) != (0, 0, 0):
            give_back(r, d, c).start()
    own_start = z_row * line + (x * 2 + core) * tokens
    parts_in[core, z_row, x] = parts_out[pl.ds(pl.multiple_of(own_start, tokens), tokens)]

    for i, r, d in feeds:
        if (r, d) == (0, 0):

            @pl.when(core != FEED_CORE)
            def _():
                feed(i, r, d).wait_send()

        else:
            feed(i, r, d).wait_send()

    @pl.when(feeds_pair)
    def _():
        for p in range(pieces):
            to_pair(own.at[p], p).wait_send()
        for h in range(heads):
            to_pair(q_heads.at[h], pieces + h).wait_send()

    def sent(step, carry):
        pltpu.make_async_copy(ring.at[step], ring.at[step], ring_send.at[step]).wait()
        return carry

    lax.fori_loop(0, steps, sent, 0)
    for r, d, c in backs:
        if (r, d, c) != (0, 0, 0):
            give_back(r, d, c).wait_send()

    local_weight.wait()
    sent_weight.wait()
    attn = []
    sources = [(c, r, d) for c in range(2) for r in range(ROWS) for d in range(COLUMNS)]
    for i, (c, r, d) in enumerate(sources):
        itself = (z_row == r) & (x == d) & (core == c)

        @pl.when(jnp.logical_not(itself))
        def _():
            part = parts_in.at[c, r, d]
            pltpu.make_async_copy(part, part, back_recv.at[i]).wait()

    for d in range(COLUMNS):
        for h in range(heads):
            part = sum(
                parts_in[c, r, d, :, h * PAD : (h + 1) * PAD].astype(f32)
                for c in range(2)
                for r in range(ROWS)
            )
            total_weight = part[:, HD : HD + 1] + part[:, HD + 16 : HD + 17]
            attn.append((part[:, 0:HD] / total_weight).astype(bf16))
    attn = jnp.concatenate(attn, axis=1)
    mixed[...] = jnp.dot(attn, whole_weight[...], preferred_element_type=f32).astype(bf16)


def on_device(lines, query, key, value, q_gain, k_gain, out_weight):
    tokens, width = query.shape
    heads = width // HD // COLUMNS
    nodes = lines // ROWS
    pieces = 2 * heads
    most = max(AHEAD, nodes - 1 - AHEAD)
    line = 2 * COLUMNS * tokens
    window = 3 * PAD
    f32, bf16 = jnp.float32, jnp.bfloat16
    hbm = pl.BlockSpec(memory_space=pl.ANY)
    vmem = pl.BlockSpec(memory_space=pltpu.VMEM)
    dma = pltpu.SemaphoreType.DMA
    return pl.pallas_call(
        functools.partial(kernel, nodes, heads),
        out_shape=jax.ShapeDtypeStruct((tokens, out_weight.shape[1]), bf16),
        in_specs=[hbm, hbm, hbm, vmem, vmem, hbm],
        out_specs=vmem,
        scratch_shapes=[
            pltpu.VMEM((3, tokens, width), bf16),
            pltpu.VMEM((line, window), bf16),
            pltpu.VMEM((line, window), bf16),
            pltpu.VMEM((ROWS, line, window), bf16),
            pltpu.VMEM((2, window, line), f32),
            pltpu.VMEM((PAD, PAD), f32),
            pltpu.VMEM((pieces, HD, line), bf16),
            pltpu.VMEM((most, pieces, HD, line), bf16),
            pltpu.VMEM((heads, ROWS * line, PAD), bf16),
            pltpu.VMEM((heads, ROWS * line, PAD), f32),
            pltpu.VMEM((ROWS * line, heads * PAD), bf16),
            pltpu.VMEM((2, ROWS, COLUMNS, tokens, heads * PAD), bf16),
            pltpu.VMEM((2 * out_weight.shape[0], out_weight.shape[1]), bf16),
            dma((3,)),
            dma(((2 + ROWS) * COLUMNS,)),
            dma((2 + ROWS,)),
            dma((most,)),
            dma((most, pieces)),
            dma((ROWS * COLUMNS * 2,)),
            dma((2 * ROWS * COLUMNS,)),
            dma((3,)),
            dma((pieces + heads,)),
            dma((pieces + heads,)),
            pltpu.SemaphoreType.REGULAR,
        ],
        compiler_params=pltpu.CompilerParams(collective_id=0, has_side_effects=True),
        name="attention",
    )(query, key, value, q_gain.reshape(1, HD), k_gain.reshape(1, HD), out_weight)


def solution(mesh):
    tokens = P(("grp", "blk", "uly"), None)
    return jax.shard_map(
        functools.partial(on_device, mesh.shape["blk"] // COLUMNS),
        mesh=mesh,
        in_specs=(tokens, tokens, tokens, P(), P(), P("uly", None)),
        out_specs=tokens,
        check_vma=False,
    )
```

```python
import functools
import math

import jax
import jax.numpy as jnp
from jax import lax
from jax.experimental import pallas as pl
from jax.experimental.pallas import tpu as pltpu
from jax.sharding import PartitionSpec as P

HD = 96
PAD = 128
COLUMNS = 4
ROWS = 2
FEED_CORE = 1
AHEAD = 5
MESH = pl.DeviceIdType.MESH
TN = (((1,), (1,)), ((), ()))


def kernel(
    nodes,
    heads,
    query,
    key,
    value,
    q_gain,
    k_gain,
    weight,
    mixed,
    stage,
    key_raw,
    value_raw,
    query_raw,
    turned,
    gain_rows,
    gain_pad,
    own,
    ring,
    q_heads,
    totals,
    parts_out,
    parts_in,
    whole_weight,
    stage_sem,
    gain_sem,
    feed_send,
    feed_recv,
    ring_send,
    ring_recv,
    back_send,
    back_recv,
    weight_sem,
    pair_send,
    pair_recv,
    ready,
):
    f32, bf16 = jnp.float32, jnp.bfloat16
    block = lax.axis_index("blk")
    core = lax.axis_index("uly")
    z, x = lax.div(block, COLUMNS), lax.rem(block, COLUMNS)
    z_block, z_row = lax.div(z, ROWS), lax.rem(z, ROWS)
    feeds_pair = core == FEED_CORE
    tokens = query.shape[0]
    window = 3 * PAD
    lanes = 2 * PAD
    group = heads * HD
    line = 2 * COLUMNS * tokens
    pieces = 2 * heads
    steps = jnp.where(feeds_pair, nodes - 1 - AHEAD, AHEAD)

    def device(row, column, a_core):
        return {"blk": row * COLUMNS + column, "uly": a_core}

    def other_row(r):
        return z_block * ROWS + lax.rem(z_row + r, ROWS)

    def other_column(d):
        return lax.rem(x + d, COLUMNS)

    node, last_node = z_block, nodes - 1
    ahead = lax.rem(z + ROWS, nodes * ROWS)
    behind = lax.rem(z + last_node * ROWS, nodes * ROWS)
    is_first, is_last = node == 0, node == last_node

    staged = [
        pltpu.make_async_copy(src, stage.at[i], stage_sem.at[i])
        for i, src in enumerate((key, value, query))
    ]
    gains = [
        pltpu.make_async_copy(src, gain_rows.at[i], gain_sem.at[i])
        for i, src in enumerate((q_gain, k_gain))
    ]
    for copy in staged + gains:
        copy.start()

    barrier = pltpu.get_barrier_semaphore()

    def greet(dev):
        pl.semaphore_signal(barrier, inc=1, device_id=dev, device_id_type=MESH)

    @pl.when(feeds_pair)
    def _():
        for r in range(ROWS):
            for d in range(COLUMNS):
                for c in range(2):
                    if (r, d, c) != (0, 0, 0):
                        greet(device(other_row(r), other_column(d), lax.rem(core + c, 2)))

    greets_ahead = jnp.where(feeds_pair, node != last_node, (node != 0) & (node != last_node))
    greets_behind = jnp.where(feeds_pair, node == 0, node < 2)
    lower = jnp.where(feeds_pair, node != 0, node != 1).astype(jnp.int32) + jnp.where(is_last, 1, 0)

    @pl.when(greets_ahead)
    def _():
        greet(device(ahead, x, core))

    @pl.when(greets_behind)
    def _():
        greet(device(behind, x, core))

    pl.semaphore_wait(barrier, ROWS * COLUMNS - jnp.where(feeds_pair, 1, 0) + lower)

    target = jnp.where(feeds_pair, behind, ahead)
    source = jnp.where(feeds_pair, ahead, behind)

    @pl.when(jnp.where(feeds_pair, node == last_node, node > 1))
    def _():
        pl.semaphore_signal(ready, inc=1, device_id=device(source, x, core), device_id_type=MESH)

    def wait_for_target():
        @pl.when(jnp.where(feeds_pair, node == 0, (node != 0) & (node != last_node)))
        def _():
            pl.semaphore_wait(ready, 1)

    place = pl.ds(pl.multiple_of((x * 2 + core) * tokens, tokens), tokens)

    def feed(i, r, d):
        column = other_column(d)
        dst = (key_raw, value_raw, query_raw.at[z_row])[i].at[place]
        recv = feed_recv.at[i] if i < 2 else feed_recv.at[2 + z_row]
        return pltpu.make_async_remote_copy(
            src_ref=stage.at[i, :, pl.ds(pl.multiple_of(column * lanes, PAD), window)],
            dst_ref=dst,
            send_sem=feed_send.at[i * COLUMNS + d if i < 2 else (2 + r) * COLUMNS + d],
            recv_sem=recv,
            device_id=device(other_row(r), column, FEED_CORE),
            device_id_type=MESH,
        )

    def own_feed(i):
        dst = (key_raw, value_raw, query_raw.at[z_row])[i].at[place]
        recv = feed_recv.at[i] if i < 2 else feed_recv.at[2 + z_row]
        src = (key, value, query)[i]
        return pltpu.make_async_copy(
            src.at[:, pl.ds(pl.multiple_of(x * lanes, PAD), window)], dst, recv
        )

    feeds = [(i, r, d) for i in range(3) for r in range(ROWS if i == 2 else 1) for d in (2, 1, 3, 0)]
    for i, r, d in feeds:
        if (r, d) == (0, 2):
            staged[i].wait()
        if (r, d) == (0, 0):

            @pl.when(feeds_pair)
            def _():
                own_feed(i).start()

            @pl.when(core != FEED_CORE)
            def _():
                feed(i, r, d).start()

        else:
            feed(i, r, d).start()

    depth = weight.shape[0]
    mine = whole_weight.at[pl.ds(pl.multiple_of(core * depth, 16), depth)]
    local_weight = pltpu.make_async_copy(weight, mine, weight_sem.at[0])
    sent_weight = pltpu.make_async_remote_copy(
        src_ref=weight,
        dst_ref=mine,
        send_sem=weight_sem.at[1],
        recv_sem=weight_sem.at[2],
        device_id=device(z, x, 1 - core),
        device_id_type=MESH,
    )
    local_weight.start()

    @pl.when(core != FEED_CORE)
    def _():
        sent_weight.start()

    def give_back(r, d, c, h):
        column, a_core = other_column(d), lax.rem(core + c, 2)
        row = lax.rem(z_row + r, ROWS)
        start = row * line + (column * 2 + a_core) * tokens
        return pltpu.make_async_remote_copy(
            src_ref=parts_out.at[h, pl.ds(pl.multiple_of(start, tokens), tokens)],
            dst_ref=parts_in.at[core, z_row, x, h],
            send_sem=back_send.at[h],
            recv_sem=back_recv.at[(core * ROWS + z_row) * COLUMNS + x],
            device_id=device(other_row(r), column, a_core),
            device_id_type=MESH,
        )

    backs = [(r, d, c) for r in range(ROWS) for d in range(COLUMNS) for c in range(2)]

    def landing(step, p, src):
        return pltpu.make_async_remote_copy(
            src_ref=src,
            dst_ref=ring.at[step, p],
            send_sem=ring_send.at[step],
            recv_sem=ring_recv.at[step, p],
            device_id=device(target, x, core),
            device_id_type=MESH,
        )

    def to_pair(ref, p):
        return pltpu.make_async_remote_copy(
            src_ref=ref,
            dst_ref=ref,
            send_sem=pair_send.at[p],
            recv_sem=pair_recv.at[p],
            device_id=device(z, x, 1 - core),
            device_id_type=MESH,
        )

    scale = float(HD) ** (-0.5) * math.log2(math.e)

    def attend(h, k, v):
        k = jnp.concatenate([k, jnp.zeros((PAD - HD, line), bf16)], axis=0)
        v = jnp.concatenate([v, jnp.ones((PAD - HD, line), bf16)], axis=0)
        scores = jnp.dot(q_heads[h], k, preferred_element_type=f32)
        expd = jnp.exp2(scores * scale).astype(bf16)
        totals[h] += lax.dot_general(expd, v, TN, preferred_element_type=f32)

    totals[...] = jnp.zeros_like(totals)

    @pl.when(feeds_pair)
    def _():
        for i in range(2):
            gains[i].wait()
            gain_pad[...] = jnp.zeros_like(gain_pad)
            gain_pad[:, 0:HD] = jnp.broadcast_to(gain_rows[i], (PAD, HD))
            turned[i, 0:PAD, :] = gain_pad[...].T
        q_column, k_column = turned[0, 0:HD, :], turned[1, 0:HD, :]
        first = x * (group - lanes)

        def head_of(i, h):
            return turned[i, pl.ds(pl.multiple_of(first + h * HD, 32), HD), :]

        def normed(data, gain):
            meansq = jnp.mean(data * data, axis=0, keepdims=True)
            return data * lax.rsqrt(meansq + 1e-06) * gain

        def send_own(kind):
            for p in range(kind * heads, (kind + 1) * heads):

                @pl.when(node != 0)
                def _():
                    landing(0, p, own.at[p]).start()

                to_pair(own.at[p], p).start()

        pltpu.make_async_copy(key_raw, key_raw, feed_recv.at[0]).wait()
        turned[0] = key_raw[...].astype(f32).T
        for h in range(heads):
            own[h] = normed(head_of(0, h), k_column).astype(bf16)
        send_own(0)
        pltpu.make_async_copy(value_raw, value_raw, feed_recv.at[1]).wait()
        turned[1] = value_raw[...].astype(f32).T
        for h in range(heads):
            own[heads + h] = head_of(1, h).astype(bf16)
        send_own(1)

        for r in range(ROWS):
            rows = query_raw.at[r]
            pltpu.make_async_copy(rows, rows, feed_recv.at[2 + r]).wait()
            turned[0] = query_raw[r].astype(f32).T
            for h in range(heads):
                data = normed(head_of(0, h), q_column)
                data = jnp.concatenate([data, jnp.zeros((PAD - HD, line), f32)], axis=0)
                q_heads[h, r * line : (r + 1) * line, :] = data.T.astype(bf16)

        for h in range(heads):
            to_pair(q_heads.at[h], pieces + h).start()
        sent_weight.start()
        for h in range(heads):
            attend(h, own[h], own[heads + h])
        wait_for_target()

        @pl.when(node == 0)
        def _():
            for p in range(pieces):
                landing(0, p, own.at[p]).start()

    @pl.when(core != FEED_CORE)
    def _():
        for copy in gains:
            copy.wait()
        wait_for_target()
        for p in range(pieces):
            to_pair(own.at[p], p).wait_recv()
            landing(0, p, own.at[p]).start()
        for h in range(heads):
            to_pair(q_heads.at[h], pieces + h).wait_recv()

    lane = lax.broadcasted_iota(jnp.int32, (ROWS * line, PAD), 1)

    def ring_step(step, last):
        for p in range(pieces):
            landing(step, p, own.at[p]).wait_recv()
            if not last:
                landing(step + 1, p, ring.at[step, p]).start()
            if p >= heads:
                h = p - heads
                attend(h, ring[step, h], ring[step, p])
                if last:
                    total = totals[h]
                    high = total.astype(bf16)
                    low = (total - high.astype(f32)).astype(bf16)
                    parts_out[h] = jnp.where(lane >= HD + 16, low, high)
                    for r, d, c in backs:
                        if (r, d, c) != (0, 0, 0):
                            give_back(r, d, c, h).start()

    def chunk(step, carry):
        ring_step(step, False)
        return carry

    lax.fori_loop(0, steps - 1, chunk, 0)
    ring_step(steps - 1, True)
    own_start = z_row * line + (x * 2 + core) * tokens
    for h in range(heads):
        parts_in[core, z_row, x, h] = parts_out[h, pl.ds(pl.multiple_of(own_start, tokens), tokens)]

    for i, r, d in feeds:
        if (r, d) == (0, 0):

            @pl.when(core != FEED_CORE)
            def _():
                feed(i, r, d).wait_send()

        else:
            feed(i, r, d).wait_send()

    @pl.when(feeds_pair)
    def _():
        for p in range(pieces):
            to_pair(own.at[p], p).wait_send()
        for h in range(heads):
            to_pair(q_heads.at[h], pieces + h).wait_send()

    def sent(step, carry):
        pltpu.make_async_copy(ring.at[step], ring.at[step], ring_send.at[step]).wait()
        return carry

    lax.fori_loop(0, steps, sent, 0)
    for h in range(heads):
        others = parts_out.at[h, 0 : (len(backs) - 1) * tokens]
        pltpu.make_async_copy(others, others, back_send.at[h]).wait()

    local_weight.wait()
    sent_weight.wait()
    attn = []
    sources = [(c, r, d) for c in range(2) for r in range(ROWS) for d in range(COLUMNS)]
    for i, (c, r, d) in enumerate(sources):
        itself = (z_row == r) & (x == d) & (core == c)

        @pl.when(jnp.logical_not(itself))
        def _():
            part = parts_in.at[c, r, d]
            pltpu.make_async_copy(part, part, back_recv.at[i]).wait()

    for d in range(COLUMNS):
        for h in range(heads):
            part = sum(
                parts_in[c, r, d, h].astype(f32)
                for c in range(2)
                for r in range(ROWS)
            )
            total_weight = part[:, HD : HD + 1] + part[:, HD + 16 : HD + 17]
            attn.append((part[:, 0:HD] / total_weight).astype(bf16))
    attn = jnp.concatenate(attn, axis=1)
    mixed[...] = jnp.dot(attn, whole_weight[...], preferred_element_type=f32).astype(bf16)


def on_device(lines, query, key, value, q_gain, k_gain, out_weight):
    tokens, width = query.shape
    heads = width // HD // COLUMNS
    nodes = lines // ROWS
    pieces = 2 * heads
    most = max(AHEAD, nodes - 1 - AHEAD)
    line = 2 * COLUMNS * tokens
    window = 3 * PAD
    f32, bf16 = jnp.float32, jnp.bfloat16
    hbm = pl.BlockSpec(memory_space=pl.ANY)
    vmem = pl.BlockSpec(memory_space=pltpu.VMEM)
    dma = pltpu.SemaphoreType.DMA
    return pl.pallas_call(
        functools.partial(kernel, nodes, heads),
        out_shape=jax.ShapeDtypeStruct((tokens, out_weight.shape[1]), bf16),
        in_specs=[hbm] * 6,
        out_specs=vmem,
        scratch_shapes=[
            pltpu.VMEM((3, tokens, width), bf16),
            pltpu.VMEM((line, window), bf16),
            pltpu.VMEM((line, window), bf16),
            pltpu.VMEM((ROWS, line, window), bf16),
            pltpu.VMEM((2, window, line), f32),
            pltpu.VMEM((2, 1, HD), f32),
            pltpu.VMEM((PAD, PAD), f32),
            pltpu.VMEM((pieces, HD, line), bf16),
            pltpu.VMEM((most, pieces, HD, line), bf16),
            pltpu.VMEM((heads, ROWS * line, PAD), bf16),
            pltpu.VMEM((heads, ROWS * line, PAD), f32),
            pltpu.VMEM((heads, ROWS * line, PAD), bf16),
            pltpu.VMEM((2, ROWS, COLUMNS, heads, tokens, PAD), bf16),
            pltpu.VMEM((2 * out_weight.shape[0], out_weight.shape[1]), bf16),
            dma((3,)),
            dma((2,)),
            dma(((2 + ROWS) * COLUMNS,)),
            dma((2 + ROWS,)),
            dma((most,)),
            dma((most, pieces)),
            dma((heads,)),
            dma((2 * ROWS * COLUMNS,)),
            dma((3,)),
            dma((pieces + heads,)),
            dma((pieces + heads,)),
            pltpu.SemaphoreType.REGULAR,
        ],
        compiler_params=pltpu.CompilerParams(collective_id=0, has_side_effects=True),
        name="attention",
    )(query, key, value, q_gain.reshape(1, HD), k_gain.reshape(1, HD), out_weight)


def solution(mesh):
    tokens = P(("grp", "blk", "uly"), None)
    return jax.shard_map(
        functools.partial(on_device, mesh.shape["blk"] // COLUMNS),
        mesh=mesh,
        in_specs=(tokens, tokens, tokens, P(), P(), P("uly", None)),
        out_specs=tokens,
        check_vma=False,
    )
```

```python
import functools
import math

import jax
import jax.numpy as jnp
from jax import lax
from jax.experimental import pallas as pl
from jax.experimental.pallas import tpu as pltpu
from jax.sharding import PartitionSpec as P

HD = 96
PAD = 128
COLUMNS = 4
ROWS = 2
FEED_CORE = 1
UP = 5
LAND = 3
MESH = pl.DeviceIdType.MESH
TN = (((1,), (1,)), ((), ()))


def kernel(
    nodes,
    heads,
    query,
    key,
    value,
    q_gain,
    k_gain,
    weight,
    mixed,
    stage,
    key_raw,
    value_raw,
    query_raw,
    turned,
    gain_rows,
    gain_pad,
    own,
    ring,
    q_heads,
    totals,
    parts_out,
    parts_in,
    whole_weight,
    stage_sem,
    gain_sem,
    feed_send,
    feed_recv,
    ring_send,
    ring_recv,
    also_send,
    express_send,
    back_send,
    back_recv,
    weight_sem,
    pair_send,
    pair_recv,
    ready,
):
    f32, bf16 = jnp.float32, jnp.bfloat16
    block = lax.axis_index("blk")
    core = lax.axis_index("uly")
    z, x = lax.div(block, COLUMNS), lax.rem(block, COLUMNS)
    z_block, z_row = lax.div(z, ROWS), lax.rem(z, ROWS)
    feeds_pair = core == FEED_CORE
    tokens = query.shape[0]
    window = 3 * PAD
    lanes = 2 * PAD
    group = heads * HD
    line = 2 * COLUMNS * tokens
    pieces = 2 * heads
    half = nodes // 2
    far = half - UP

    def device(row, column, a_core):
        return {"blk": row * COLUMNS + column, "uly": a_core}

    def other_row(r):
        return z_block * ROWS + lax.rem(z_row + r, ROWS)

    def other_column(d):
        return lax.rem(x + d, COLUMNS)

    node, last_node = z_block, nodes - 1
    ahead = lax.rem(z + ROWS, nodes * ROWS)
    behind = lax.rem(z + last_node * ROWS, nodes * ROWS)
    is_first, is_last = node == 0, node == last_node
    is_low = node < half
    express = feeds_pair & (node >= half) & (node < half + far)

    steps = jnp.where(
        feeds_pair,
        jnp.where(node <= LAND, half + far - 1 - node, jnp.where(is_low, half - 1 - node, half)),
        jnp.where(node <= LAND, node + UP, jnp.where(is_low, node + half, half - 1)),
    )

    def passes(slot):
        owner = lax.rem(node + 1 + slot, nodes)
        down = jnp.where(
            owner < half, slot + 2 <= half, (node > half) | ((node <= LAND) & (node >= 1))
        )
        low_owner = slot < node
        up = jnp.where(
            is_low,
            jnp.where(node + 1 < half, True, low_owner & (slot + 2 <= half - 1)),
            jnp.where(is_last, slot + 2 <= UP, slot + 2 <= half - 1),
        )
        skip = jnp.where(~feeds_pair & (node == LAND) & (slot >= node), far, 0)
        return jnp.where(feeds_pair, down, up), slot + 1 + skip

    def passes_over(slot):
        owner = node + 1 + slot
        return feeds_pair & (node == LAND) & (owner >= half), owner - half + LAND + 1

    staged = [
        pltpu.make_async_copy(src, stage.at[i], stage_sem.at[i])
        for i, src in enumerate((key, value, query))
    ]
    gains = [
        pltpu.make_async_copy(src, gain_rows.at[i], gain_sem.at[i])
        for i, src in enumerate((q_gain, k_gain))
    ]
    for copy in staged + gains:
        copy.start()

    barrier = pltpu.get_barrier_semaphore()

    def greet(dev):
        pl.semaphore_signal(barrier, inc=1, device_id=dev, device_id_type=MESH)

    @pl.when(feeds_pair)
    def _():
        for r in range(ROWS):
            for d in range(COLUMNS):
                for c in range(2):
                    if (r, d, c) != (0, 0, 0):
                        greet(device(other_row(r), other_column(d), lax.rem(core + c, 2)))

    greets_ahead = jnp.where(feeds_pair, node != last_node, (node != 0) & (node != last_node))
    greets_behind = jnp.where(feeds_pair, node == 0, node < 2)
    lower = jnp.where(feeds_pair, node != 0, node != 1).astype(jnp.int32) + jnp.where(is_last, 1, 0)
    lower = lower + jnp.where(express, 1, 0)

    @pl.when(greets_ahead)
    def _():
        greet(device(ahead, x, core))

    @pl.when(greets_behind)
    def _():
        greet(device(behind, x, core))

    @pl.when(feeds_pair & (node == LAND))
    def _():
        for i in range(far):
            greet(device((half + i) * ROWS + z_row, x, core))

    pl.semaphore_wait(barrier, ROWS * COLUMNS - jnp.where(feeds_pair, 1, 0) + lower)

    target = jnp.where(feeds_pair, behind, ahead)
    source = jnp.where(feeds_pair, ahead, behind)

    @pl.when(jnp.where(feeds_pair, node == last_node, node > 1))
    def _():
        pl.semaphore_signal(ready, inc=1, device_id=device(source, x, core), device_id_type=MESH)

    def wait_for_target():
        @pl.when(jnp.where(feeds_pair, node == 0, (node != 0) & (node != last_node)))
        def _():
            pl.semaphore_wait(ready, 1)

    place = pl.ds(pl.multiple_of((x * 2 + core) * tokens, tokens), tokens)

    def feed(i, r, d):
        column = other_column(d)
        dst = (key_raw, value_raw, query_raw.at[z_row])[i].at[place]
        recv = feed_recv.at[i] if i < 2 else feed_recv.at[2 + z_row]
        return pltpu.make_async_remote_copy(
            src_ref=stage.at[i, :, pl.ds(pl.multiple_of(column * lanes, PAD), window)],
            dst_ref=dst,
            send_sem=feed_send.at[i * COLUMNS + d if i < 2 else (2 + r) * COLUMNS + d],
            recv_sem=recv,
            device_id=device(other_row(r), column, FEED_CORE),
            device_id_type=MESH,
        )

    def own_feed(i):
        dst = (key_raw, value_raw, query_raw.at[z_row])[i].at[place]
        recv = feed_recv.at[i] if i < 2 else feed_recv.at[2 + z_row]
        src = (key, value, query)[i]
        return pltpu.make_async_copy(
            src.at[:, pl.ds(pl.multiple_of(x * lanes, PAD), window)], dst, recv
        )

    feeds = [(i, r, d) for i in range(3) for r in range(ROWS if i == 2 else 1) for d in (2, 1, 3, 0)]
    for i, r, d in feeds:
        if (r, d) == (0, 2):
            staged[i].wait()
        if (r, d) == (0, 0):

            @pl.when(feeds_pair)
            def _():
                own_feed(i).start()

            @pl.when(core != FEED_CORE)
            def _():
                feed(i, r, d).start()

        else:
            feed(i, r, d).start()

    depth = weight.shape[0]
    mine = whole_weight.at[pl.ds(pl.multiple_of(core * depth, 16), depth)]
    local_weight = pltpu.make_async_copy(weight, mine, weight_sem.at[0])
    sent_weight = pltpu.make_async_remote_copy(
        src_ref=weight,
        dst_ref=mine,
        send_sem=weight_sem.at[1],
        recv_sem=weight_sem.at[2],
        device_id=device(z, x, 1 - core),
        device_id_type=MESH,
    )
    local_weight.start()

    @pl.when(core != FEED_CORE)
    def _():
        sent_weight.start()

    def give_back(r, d, c, h):
        column, a_core = other_column(d), lax.rem(core + c, 2)
        row = lax.rem(z_row + r, ROWS)
        start = row * line + (column * 2 + a_core) * tokens
        return pltpu.make_async_remote_copy(
            src_ref=parts_out.at[h, pl.ds(pl.multiple_of(start, tokens), tokens)],
            dst_ref=parts_in.at[core, z_row, x, h],
            send_sem=back_send.at[h],
            recv_sem=back_recv.at[(core * ROWS + z_row) * COLUMNS + x],
            device_id=device(other_row(r), column, a_core),
            device_id_type=MESH,
        )

    backs = [(r, d, c) for r in range(ROWS) for d in range(COLUMNS) for c in range(2)]

    most = ring.shape[0]

    def landing(src, p, slot, dev, send_sem):
        return pltpu.make_async_remote_copy(
            src_ref=src.at[p],
            dst_ref=ring.at[slot, p],
            send_sem=send_sem,
            recv_sem=ring_recv.at[slot, p],
            device_id=dev,
            device_id_type=MESH,
        )

    def own_on(p):
        return landing(own, p, 0, device(target, x, core), ring_send.at[most])

    def own_express(p):
        there = device(LAND * ROWS + z_row, x, core)
        return landing(own, p, node - LAND - 1, there, express_send)

    def passed(p, slot):
        return landing(
            ring.at[slot], p, passes(slot)[1], device(target, x, core), ring_send.at[slot]
        )

    def passed_over(p, slot):
        return landing(
            ring.at[slot], p, passes_over(slot)[1], device(ahead, x, 1 - core), also_send.at[slot]
        )

    def to_pair(ref, p):
        return pltpu.make_async_remote_copy(
            src_ref=ref,
            dst_ref=ref,
            send_sem=pair_send.at[p],
            recv_sem=pair_recv.at[p],
            device_id=device(z, x, 1 - core),
            device_id_type=MESH,
        )

    scale = float(HD) ** (-0.5) * math.log2(math.e)

    def attend(h, k, v):
        k = jnp.concatenate([k, jnp.zeros((PAD - HD, line), bf16)], axis=0)
        v = jnp.concatenate([v, jnp.ones((PAD - HD, line), bf16)], axis=0)
        scores = jnp.dot(q_heads[h], k, preferred_element_type=f32)
        expd = jnp.exp2(scores * scale).astype(bf16)
        totals[h] += lax.dot_general(expd, v, TN, preferred_element_type=f32)

    totals[...] = jnp.zeros_like(totals)

    @pl.when(feeds_pair)
    def _():
        for i in range(2):
            gains[i].wait()
            gain_pad[...] = jnp.zeros_like(gain_pad)
            gain_pad[:, 0:HD] = jnp.broadcast_to(gain_rows[i], (PAD, HD))
            turned[i, 0:PAD, :] = gain_pad[...].T
        q_column, k_column = turned[0, 0:HD, :], turned[1, 0:HD, :]
        first = x * (group - lanes)

        def head_of(i, h):
            return turned[i, pl.ds(pl.multiple_of(first + h * HD, 32), HD), :]

        def normed(data, gain):
            meansq = jnp.mean(data * data, axis=0, keepdims=True)
            return data * lax.rsqrt(meansq + 1e-06) * gain

        def send_own(kind):
            mine = range(kind * heads, (kind + 1) * heads)

            @pl.when(express)
            def _():
                for p in mine:
                    own_express(p).start()

            @pl.when((node != 0) & (node != half))
            def _():
                for p in mine:
                    own_on(p).start()

            for p in mine:
                to_pair(own.at[p], p).start()

        pltpu.make_async_copy(key_raw, key_raw, feed_recv.at[0]).wait()
        turned[0] = key_raw[...].astype(f32).T
        for h in range(heads):
            own[h] = normed(head_of(0, h), k_column).astype(bf16)
        send_own(0)
        pltpu.make_async_copy(value_raw, value_raw, feed_recv.at[1]).wait()
        turned[1] = value_raw[...].astype(f32).T
        for h in range(heads):
            own[heads + h] = head_of(1, h).astype(bf16)
        send_own(1)

        for r in range(ROWS):
            rows = query_raw.at[r]
            pltpu.make_async_copy(rows, rows, feed_recv.at[2 + r]).wait()
            turned[0] = query_raw[r].astype(f32).T
            for h in range(heads):
                data = normed(head_of(0, h), q_column)
                data = jnp.concatenate([data, jnp.zeros((PAD - HD, line), f32)], axis=0)
                q_heads[h, r * line : (r + 1) * line, :] = data.T.astype(bf16)

        for h in range(heads):
            to_pair(q_heads.at[h], pieces + h).start()
        sent_weight.start()
        for h in range(heads):
            attend(h, own[h], own[heads + h])
        wait_for_target()

        @pl.when(node == 0)
        def _():
            for p in range(pieces):
                own_on(p).start()

    @pl.when(core != FEED_CORE)
    def _():
        for copy in gains:
            copy.wait()
        wait_for_target()
        for p in range(pieces):
            to_pair(own.at[p], p).wait_recv()
            own_on(p).start()
        for h in range(heads):
            to_pair(q_heads.at[h], pieces + h).wait_recv()

    lane = lax.broadcasted_iota(jnp.int32, (ROWS * line, PAD), 1)

    def give(h):
        total = totals[h]
        high = total.astype(bf16)
        low = (total - high.astype(f32)).astype(bf16)
        parts_out[h] = jnp.where(lane >= HD + 16, low, high)
        for r, d, c in backs:
            if (r, d, c) != (0, 0, 0):
                give_back(r, d, c, h).start()

    def ring_step(slot, last):
        for p in range(pieces):
            landing(own, p, slot, device(target, x, core), ring_send.at[slot]).wait_recv()

            @pl.when(passes(slot)[0])
            def _():
                passed(p, slot).start()

            @pl.when(passes_over(slot)[0])
            def _():
                passed_over(p, slot).start()

            if p >= heads:
                h = p - heads
                attend(h, ring[slot, h], ring[slot, p])
                if last:
                    give(h)

    def chunk(slot, carry):
        ring_step(slot, False)
        return carry

    lax.fori_loop(0, steps - 1, chunk, 0)

    @pl.when(steps > 0)
    def _():
        ring_step(steps - 1, True)

    @pl.when(steps == 0)
    def _():
        for h in range(heads):
            give(h)

    own_start = z_row * line + (x * 2 + core) * tokens
    for h in range(heads):
        parts_in[core, z_row, x, h] = parts_out[h, pl.ds(pl.multiple_of(own_start, tokens), tokens)]

    for i, r, d in feeds:
        if (r, d) == (0, 0):

            @pl.when(core != FEED_CORE)
            def _():
                feed(i, r, d).wait_send()

        else:
            feed(i, r, d).wait_send()

    @pl.when(feeds_pair)
    def _():
        for p in range(pieces):
            to_pair(own.at[p], p).wait_send()
        for h in range(heads):
            to_pair(q_heads.at[h], pieces + h).wait_send()

    @pl.when(express)
    def _():
        pltpu.make_async_copy(own, own, express_send).wait()

    @pl.when(jnp.logical_not(feeds_pair & (node == half)))
    def _():
        pltpu.make_async_copy(own, own, ring_send.at[most]).wait()

    def sent(slot, carry):
        @pl.when(passes(slot)[0])
        def _():
            pltpu.make_async_copy(ring.at[slot], ring.at[slot], ring_send.at[slot]).wait()

        @pl.when(passes_over(slot)[0])
        def _():
            pltpu.make_async_copy(ring.at[slot], ring.at[slot], also_send.at[slot]).wait()

        return carry

    lax.fori_loop(0, steps, sent, 0)
    for h in range(heads):
        others = parts_out.at[h, 0 : (len(backs) - 1) * tokens]
        pltpu.make_async_copy(others, others, back_send.at[h]).wait()

    local_weight.wait()
    sent_weight.wait()
    attn = []
    sources = [(c, r, d) for c in range(2) for r in range(ROWS) for d in range(COLUMNS)]
    for i, (c, r, d) in enumerate(sources):
        itself = (z_row == r) & (x == d) & (core == c)

        @pl.when(jnp.logical_not(itself))
        def _():
            part = parts_in.at[c, r, d]
            pltpu.make_async_copy(part, part, back_recv.at[i]).wait()

    for d in range(COLUMNS):
        for h in range(heads):
            part = sum(
                parts_in[c, r, d, h].astype(f32)
                for c in range(2)
                for r in range(ROWS)
            )
            total_weight = part[:, HD : HD + 1] + part[:, HD + 16 : HD + 17]
            attn.append((part[:, 0:HD] / total_weight).astype(bf16))
    attn = jnp.concatenate(attn, axis=1)
    mixed[...] = jnp.dot(attn, whole_weight[...], preferred_element_type=f32).astype(bf16)


def on_device(lines, query, key, value, q_gain, k_gain, out_weight):
    tokens, width = query.shape
    heads = width // HD // COLUMNS
    nodes = lines // ROWS
    pieces = 2 * heads
    most = nodes - 1
    line = 2 * COLUMNS * tokens
    window = 3 * PAD
    f32, bf16 = jnp.float32, jnp.bfloat16
    hbm = pl.BlockSpec(memory_space=pl.ANY)
    vmem = pl.BlockSpec(memory_space=pltpu.VMEM)
    dma = pltpu.SemaphoreType.DMA
    return pl.pallas_call(
        functools.partial(kernel, nodes, heads),
        out_shape=pltpu.VMEM((tokens, out_weight.shape[1]), bf16),
        in_specs=[hbm] * 6,
        out_specs=vmem,
        scratch_shapes=[
            pltpu.VMEM((3, tokens, width), bf16),
            pltpu.VMEM((line, window), bf16),
            pltpu.VMEM((line, window), bf16),
            pltpu.VMEM((ROWS, line, window), bf16),
            pltpu.VMEM((2, window, line), f32),
            pltpu.VMEM((2, 1, HD), f32),
            pltpu.VMEM((PAD, PAD), f32),
            pltpu.VMEM((pieces, HD, line), bf16),
            pltpu.VMEM((most, pieces, HD, line), bf16),
            pltpu.VMEM((heads, ROWS * line, PAD), bf16),
            pltpu.VMEM((heads, ROWS * line, PAD), f32),
            pltpu.VMEM((heads, ROWS * line, PAD), bf16),
            pltpu.VMEM((2, ROWS, COLUMNS, heads, tokens, PAD), bf16),
            pltpu.VMEM((2 * out_weight.shape[0], out_weight.shape[1]), bf16),
            dma((3,)),
            dma((2,)),
            dma(((2 + ROWS) * COLUMNS,)),
            dma((2 + ROWS,)),
            dma((most + 1,)),
            dma((most, pieces)),
            dma((most,)),
            dma,
            dma((heads,)),
            dma((2 * ROWS * COLUMNS,)),
            dma((3,)),
            dma((pieces + heads,)),
            dma((pieces + heads,)),
            pltpu.SemaphoreType.REGULAR,
        ],
        compiler_params=pltpu.CompilerParams(collective_id=0, has_side_effects=True),
        name="attention",
    )(query, key, value, q_gain.reshape(1, HD), k_gain.reshape(1, HD), out_weight)


def solution(mesh):
    tokens = P(("grp", "blk", "uly"), None)
    return jax.shard_map(
        functools.partial(on_device, mesh.shape["blk"] // COLUMNS),
        mesh=mesh,
        in_specs=(tokens, tokens, tokens, P(), P(), P("uly", None)),
        out_specs=tokens,
        check_vma=False,
    )
```

```python
import functools
import math

import jax
import jax.numpy as jnp
from jax import lax
from jax.experimental import pallas as pl
from jax.experimental.pallas import tpu as pltpu
from jax.sharding import PartitionSpec as P

HD = 96
PAD = 128
COLUMNS = 4
ROWS = 2
FEED_CORE = 1
AHEAD = 7
HEADS_UP = 1
MESH = pl.DeviceIdType.MESH
TN = (((1,), (1,)), ((), ()))


def kernel(
    nodes,
    heads,
    query,
    key,
    value,
    q_gain,
    k_gain,
    weight,
    mixed,
    stage,
    key_raw,
    value_raw,
    query_raw,
    turned,
    gain_rows,
    gain_pad,
    own,
    ring,
    q_heads,
    totals,
    parts_out,
    parts_in,
    whole_weight,
    stage_sem,
    gain_sem,
    feed_send,
    feed_recv,
    ring_send,
    ring_recv,
    back_send,
    back_recv,
    weight_sem,
    pair_send,
    pair_recv,
    ready,
):
    f32, bf16 = jnp.float32, jnp.bfloat16
    block = lax.axis_index("blk")
    core = lax.axis_index("uly")
    z, x = lax.div(block, COLUMNS), lax.rem(block, COLUMNS)
    z_block, z_row = lax.div(z, ROWS), lax.rem(z, ROWS)
    feeds_pair = core == FEED_CORE
    tokens = query.shape[0]
    window = 3 * PAD
    lanes = 2 * PAD
    group = heads * HD
    line = 2 * COLUMNS * tokens
    pieces = 2 * heads
    steps = jnp.where(feeds_pair, nodes - AHEAD, AHEAD)

    def device(row, column, a_core):
        return {"blk": row * COLUMNS + column, "uly": a_core}

    def other_row(r):
        return z_block * ROWS + lax.rem(z_row + r, ROWS)

    def other_column(d):
        return lax.rem(x + d, COLUMNS)

    node, last_node = z_block, nodes - 1
    ahead = lax.rem(z + ROWS, nodes * ROWS)
    behind = lax.rem(z + last_node * ROWS, nodes * ROWS)
    is_first, is_last = node == 0, node == last_node

    staged = [
        pltpu.make_async_copy(src, stage.at[i], stage_sem.at[i])
        for i, src in enumerate((key, value, query))
    ]
    gains = [
        pltpu.make_async_copy(src, gain_rows.at[i], gain_sem.at[i])
        for i, src in enumerate((q_gain, k_gain))
    ]
    for copy in staged + gains:
        copy.start()

    barrier = pltpu.get_barrier_semaphore()

    def greet(dev):
        pl.semaphore_signal(barrier, inc=1, device_id=dev, device_id_type=MESH)

    @pl.when(feeds_pair)
    def _():
        for r in range(ROWS):
            for d in range(COLUMNS):
                for c in range(2):
                    if (r, d, c) != (0, 0, 0):
                        greet(device(other_row(r), other_column(d), lax.rem(core + c, 2)))

    greets_ahead = jnp.where(feeds_pair, node != last_node, (node != 0) & (node != last_node))
    greets_behind = jnp.where(feeds_pair, node == 0, node < 2)
    lower = jnp.where(feeds_pair, node != 0, node != 1).astype(jnp.int32) + jnp.where(is_last, 1, 0)
    over_wrap = feeds_pair & is_last
    lower = lower + jnp.where(over_wrap, 1, 0)

    @pl.when(greets_ahead)
    def _():
        greet(device(ahead, x, core))

    @pl.when(greets_behind)
    def _():
        greet(device(behind, x, core))

    @pl.when(is_first & ~feeds_pair)
    def _():
        greet(device(behind, x, FEED_CORE))

    pl.semaphore_wait(barrier, ROWS * COLUMNS - jnp.where(feeds_pair, 1, 0) + lower)

    target = jnp.where(feeds_pair, behind, ahead)
    source = jnp.where(feeds_pair, ahead, behind)

    @pl.when(jnp.where(feeds_pair, node == last_node, node > 1))
    def _():
        pl.semaphore_signal(ready, inc=1, device_id=device(source, x, core), device_id_type=MESH)

    def wait_for_target():
        @pl.when(jnp.where(feeds_pair, node == 0, (node != 0) & (node != last_node)))
        def _():
            pl.semaphore_wait(ready, 1)

    place = pl.ds(pl.multiple_of((x * 2 + core) * tokens, tokens), tokens)

    def feed(i, r, d):
        column = other_column(d)
        dst = (key_raw, value_raw, query_raw.at[z_row])[i].at[place]
        recv = feed_recv.at[i] if i < 2 else feed_recv.at[2 + z_row]
        return pltpu.make_async_remote_copy(
            src_ref=stage.at[i, :, pl.ds(pl.multiple_of(column * lanes, PAD), window)],
            dst_ref=dst,
            send_sem=feed_send.at[i // 2],
            recv_sem=recv,
            device_id=device(other_row(r), column, FEED_CORE),
            device_id_type=MESH,
        )

    def own_feed(i):
        dst = (key_raw, value_raw, query_raw.at[z_row])[i].at[place]
        recv = feed_recv.at[i] if i < 2 else feed_recv.at[2 + z_row]
        src = (key, value, query)[i]
        return pltpu.make_async_copy(
            src.at[:, pl.ds(pl.multiple_of(x * lanes, PAD), window)], dst, recv
        )

    feeds = [(i, r, d) for i in range(3) for r in range(ROWS if i == 2 else 1) for d in (2, 1, 3, 0)]
    for i, r, d in feeds:
        if (r, d) == (0, 2):
            staged[i].wait()
        if (r, d) == (0, 0):

            @pl.when(feeds_pair)
            def _():
                own_feed(i).start()

            @pl.when(core != FEED_CORE)
            def _():
                feed(i, r, d).start()

        else:
            feed(i, r, d).start()

    depth = weight.shape[0]
    mine = whole_weight.at[pl.ds(pl.multiple_of(core * depth, 16), depth)]
    local_weight = pltpu.make_async_copy(weight, mine, weight_sem.at[0])
    sent_weight = pltpu.make_async_remote_copy(
        src_ref=weight,
        dst_ref=mine,
        send_sem=weight_sem.at[1],
        recv_sem=weight_sem.at[2],
        device_id=device(z, x, 1 - core),
        device_id_type=MESH,
    )
    local_weight.start()

    @pl.when(core != FEED_CORE)
    def _():
        sent_weight.start()

    def give_back(r, d, c):
        column, a_core = other_column(d), lax.rem(core + c, 2)
        row = lax.rem(z_row + r, ROWS)
        start = row * line + (column * 2 + a_core) * tokens
        return pltpu.make_async_remote_copy(
            src_ref=parts_out.at[pl.ds(pl.multiple_of(start, tokens), tokens)],
            dst_ref=parts_in.at[(core * ROWS + z_row) * COLUMNS + x],
            send_sem=back_send,
            recv_sem=back_recv,
            device_id=device(other_row(r), column, a_core),
            device_id_type=MESH,
        )

    backs = [(r, d, c) for r in range(ROWS) for d in range(COLUMNS) for c in range(2)]

    def landing(src, p, step, dev, send_sem):
        return pltpu.make_async_remote_copy(
            src_ref=src.at[p],
            dst_ref=ring.at[step, p],
            send_sem=send_sem,
            recv_sem=ring_recv.at[step, p],
            device_id=dev,
            device_id_type=MESH,
        )

    next_node = device(target, x, core)

    def own_on(p):
        return landing(own, p, 0, next_node, ring_send.at[0])

    def own_over_wrap(p):
        return landing(own, p, 0, device(ahead, x, 1 - core), ring_send.at[2])

    def comes_last(h):
        return feeds_pair if h >= HEADS_UP else ~feeds_pair

    def to_pair(ref, p):
        return pltpu.make_async_remote_copy(
            src_ref=ref,
            dst_ref=ref,
            send_sem=pair_send.at[p // pieces],
            recv_sem=pair_recv.at[p],
            device_id=device(z, x, 1 - core),
            device_id_type=MESH,
        )

    scale = float(HD) ** (-0.5) * math.log2(math.e)

    def attend(h, k, v):
        k = jnp.concatenate([k, jnp.zeros((PAD - HD, line), bf16)], axis=0)
        v = jnp.concatenate([v, jnp.ones((PAD - HD, line), bf16)], axis=0)
        scores = jnp.dot(q_heads[h], k, preferred_element_type=f32)
        expd = jnp.exp2(scores * scale).astype(bf16)
        totals[h] += lax.dot_general(expd, v, TN, preferred_element_type=f32)

    totals[...] = jnp.zeros_like(totals)

    @pl.when(feeds_pair)
    def _():
        for i in range(2):
            gains[i].wait()
            gain_pad[...] = jnp.zeros_like(gain_pad)
            gain_pad[:, 0:HD] = jnp.broadcast_to(gain_rows[i], (PAD, HD))
            turned[i, 0:PAD, :] = gain_pad[...].T
        q_column, k_column = turned[0, 0:HD, :], turned[1, 0:HD, :]
        first = x * (group - lanes)

        def head_of(i, h):
            return turned[i, pl.ds(pl.multiple_of(first + h * HD, 32), HD), :]

        def normed(data, gain):
            meansq = jnp.mean(data * data, axis=0, keepdims=True)
            return data * lax.rsqrt(meansq + 1e-06) * gain

        def send_own(kind):
            mine = range(kind * heads, (kind + 1) * heads)

            @pl.when(is_last)
            def _():
                for p in mine:
                    own_over_wrap(p).start()

            @pl.when(node != 0)
            def _():
                for p in mine:
                    own_on(p).start()

            @pl.when(jnp.logical_not(is_last))
            def _():
                for p in mine:
                    to_pair(own.at[p], p).start()

        pltpu.make_async_copy(key_raw, key_raw, feed_recv.at[0]).wait()
        turned[0] = key_raw[...].astype(f32).T
        for h in range(heads):
            own[h] = normed(head_of(0, h), k_column).astype(bf16)
        send_own(0)
        pltpu.make_async_copy(value_raw, value_raw, feed_recv.at[1]).wait()
        turned[1] = value_raw[...].astype(f32).T
        for h in range(heads):
            own[heads + h] = head_of(1, h).astype(bf16)
        send_own(1)

        for r in range(ROWS):
            rows = query_raw.at[r]
            pltpu.make_async_copy(rows, rows, feed_recv.at[2 + r]).wait()
            turned[0] = query_raw[r].astype(f32).T
            for h in range(heads):
                data = normed(head_of(0, h), q_column)
                data = jnp.concatenate([data, jnp.zeros((PAD - HD, line), f32)], axis=0)
                q_heads[h, r * line : (r + 1) * line, :] = data.T.astype(bf16)

        to_pair(q_heads, pieces).start()
        sent_weight.start()
        for h in range(heads):
            attend(h, own[h], own[heads + h])
        wait_for_target()

        @pl.when(node == 0)
        def _():
            for p in range(pieces):
                own_on(p).start()

    @pl.when(core != FEED_CORE)
    def _():
        for copy in gains:
            copy.wait()
        wait_for_target()

        @pl.when(jnp.logical_not(is_last))
        def _():
            for p in range(pieces):
                to_pair(own.at[p], p).wait_recv()
                own_on(p).start()

        to_pair(q_heads, pieces).wait_recv()

    lane = lax.broadcasted_iota(jnp.int32, (ROWS * line, PAD), 1)

    def arrives(step, p):
        landing(own, p, step, next_node, ring_send.at[0]).wait_recv()

    def chunk(step, carry):
        for p in range(pieces):
            arrives(step, p)

            @pl.when(step < steps - 2)
            def _():
                landing(ring.at[step], p, step + 1, next_node, ring_send.at[0]).start()

            @pl.when((step == steps - 2) & comes_last(p % heads))
            def _():
                landing(ring.at[step], p, step + 1, next_node, ring_send.at[1]).start()

            if p >= heads:
                attend(p - heads, ring[step, p - heads], ring[step, p])
        return carry

    lax.fori_loop(0, steps - 1, chunk, 0)
    for h in range(heads):

        @pl.when(comes_last(h))
        def _():
            arrives(steps - 1, h)
            arrives(steps - 1, heads + h)
            attend(h, ring[steps - 1, h], ring[steps - 1, heads + h])

        total = totals[h]
        high = total.astype(bf16)
        low = (total - high.astype(f32)).astype(bf16)
        parts_out[:, h * PAD : (h + 1) * PAD] = jnp.where(lane >= HD + 16, low, high)

    for r, d, c in backs:
        if (r, d, c) != (0, 0, 0):
            give_back(r, d, c).start()
    own_start = z_row * line + (x * 2 + core) * tokens
    parts_in[(core * ROWS + z_row) * COLUMNS + x] = parts_out[
        pl.ds(pl.multiple_of(own_start, tokens), tokens)
    ]

    def left(ref, sem):
        pltpu.make_async_copy(ref, ref, sem).wait()

    @pl.when(feeds_pair)
    def _():
        ways = COLUMNS - 1
        left(key_raw.at[0 : 2 * ways * tokens], feed_send.at[0])
        left(key_raw.at[0 : (ROWS * COLUMNS - 1) * tokens], feed_send.at[1])
        left(q_heads, pair_send.at[1])
        left(ring.at[0 : nodes - AHEAD - 1], ring_send.at[0])
        left(ring.at[0, 0 : 2 * (heads - HEADS_UP)], ring_send.at[1])

        @pl.when(is_last)
        def _():
            left(own, ring_send.at[2])

        @pl.when(jnp.logical_not(is_last))
        def _():
            left(own, pair_send.at[0])

    @pl.when(core != FEED_CORE)
    def _():
        left(key_raw.at[0 : 2 * COLUMNS * tokens], feed_send.at[0])
        left(key_raw.at[0 : ROWS * COLUMNS * tokens], feed_send.at[1])
        left(ring.at[0, 0 : 2 * HEADS_UP], ring_send.at[1])

        @pl.when(is_last)
        def _():
            left(ring.at[0 : AHEAD - 2], ring_send.at[0])

        @pl.when(jnp.logical_not(is_last))
        def _():
            left(ring.at[0 : AHEAD - 1], ring_send.at[0])

    left(parts_out.at[0 : (len(backs) - 1) * tokens], back_send)

    local_weight.wait()
    sent_weight.wait()
    attn = []
    others = parts_in.at[0 : len(backs) - 1]
    pltpu.make_async_copy(others, others, back_recv).wait()
    for d in range(COLUMNS):
        for h in range(heads):
            part = sum(
                parts_in[i * COLUMNS + d, :, h * PAD : (h + 1) * PAD].astype(f32)
                for i in range(2 * ROWS)
            )
            total_weight = part[:, HD : HD + 1] + part[:, HD + 16 : HD + 17]
            attn.append((part[:, 0:HD] / total_weight).astype(bf16))
    attn = jnp.concatenate(attn, axis=1)
    mixed[...] = jnp.dot(attn, whole_weight[...], preferred_element_type=f32).astype(bf16)


def on_device(lines, query, key, value, q_gain, k_gain, out_weight):
    tokens, width = query.shape
    heads = width // HD // COLUMNS
    nodes = lines // ROWS
    pieces = 2 * heads
    most = max(AHEAD, nodes - AHEAD)
    line = 2 * COLUMNS * tokens
    window = 3 * PAD
    f32, bf16 = jnp.float32, jnp.bfloat16
    hbm = pl.BlockSpec(memory_space=pl.ANY)
    vmem = pl.BlockSpec(memory_space=pltpu.VMEM)
    dma = pltpu.SemaphoreType.DMA
    return pl.pallas_call(
        functools.partial(kernel, nodes, heads),
        out_shape=pltpu.VMEM((tokens, out_weight.shape[1]), bf16),
        in_specs=[hbm] * 6,
        out_specs=vmem,
        scratch_shapes=[
            pltpu.VMEM((3, tokens, width), bf16),
            pltpu.VMEM((line, window), bf16),
            pltpu.VMEM((line, window), bf16),
            pltpu.VMEM((ROWS, line, window), bf16),
            pltpu.VMEM((2, window, line), f32),
            pltpu.VMEM((2, 1, HD), f32),
            pltpu.VMEM((PAD, PAD), f32),
            pltpu.VMEM((pieces, HD, line), bf16),
            pltpu.VMEM((most, pieces, HD, line), bf16),
            pltpu.VMEM((heads, ROWS * line, PAD), bf16),
            pltpu.VMEM((heads, ROWS * line, PAD), f32),
            pltpu.VMEM((ROWS * line, heads * PAD), bf16),
            pltpu.VMEM((2 * ROWS * COLUMNS, tokens, heads * PAD), bf16),
            pltpu.VMEM((2 * out_weight.shape[0], out_weight.shape[1]), bf16),
            dma((3,)),
            dma((2,)),
            dma((2,)),
            dma((2 + ROWS,)),
            dma((3,)),
            dma((most, pieces)),
            dma,
            dma,
            dma((3,)),
            dma((2,)),
            dma((pieces + 1,)),
            pltpu.SemaphoreType.REGULAR,
        ],
        compiler_params=pltpu.CompilerParams(collective_id=0, has_side_effects=True),
        name="attention",
    )(query, key, value, q_gain.reshape(1, HD), k_gain.reshape(1, HD), out_weight)


def solution(mesh):
    tokens = P(("grp", "blk", "uly"), None)
    return jax.shard_map(
        functools.partial(on_device, mesh.shape["blk"] // COLUMNS),
        mesh=mesh,
        in_specs=(tokens, tokens, tokens, P(), P(), P("uly", None)),
        out_specs=tokens,
        check_vma=False,
    )
```

```python
import functools
import math

import jax
import jax.numpy as jnp
from jax import lax
from jax.experimental import pallas as pl
from jax.experimental.pallas import tpu as pltpu
from jax.sharding import PartitionSpec as P

HD = 96
PAD = 128
COLUMNS = 4
ROWS = 2
FEED_CORE = 1
AHEAD = 7
HEADS_UP = 1
MESH = pl.DeviceIdType.MESH
TN = (((1,), (1,)), ((), ()))


def kernel(
    nodes,
    heads,
    query,
    key,
    value,
    q_gain,
    k_gain,
    weight,
    mixed,
    stage,
    key_raw,
    value_raw,
    query_raw,
    turned,
    gain_rows,
    gain_pad,
    own,
    ring,
    q_heads,
    totals,
    parts_out,
    parts_in,
    whole_weight,
    stage_sem,
    gain_sem,
    feed_send,
    feed_recv,
    ring_send,
    ring_recv,
    back_send,
    back_recv,
    weight_sem,
    pair_send,
    pair_recv,
    ready,
):
    f32, bf16 = jnp.float32, jnp.bfloat16
    block = lax.axis_index("blk")
    core = lax.axis_index("uly")
    z, x = lax.div(block, COLUMNS), lax.rem(block, COLUMNS)
    z_block, z_row = lax.div(z, ROWS), lax.rem(z, ROWS)
    feeds_pair = core == FEED_CORE
    tokens = query.shape[0]
    window = 3 * PAD
    lanes = 2 * PAD
    group = heads * HD
    line = 2 * COLUMNS * tokens
    pieces = 2 * heads
    steps = jnp.where(feeds_pair, nodes - AHEAD, AHEAD)

    def device(row, column, a_core):
        return {"blk": row * COLUMNS + column, "uly": a_core}

    def other_row(r):
        return z_block * ROWS + lax.rem(z_row + r, ROWS)

    def other_column(d):
        return lax.rem(x + d, COLUMNS)

    node, last_node = z_block, nodes - 1
    ahead = lax.rem(z + ROWS, nodes * ROWS)
    behind = lax.rem(z + last_node * ROWS, nodes * ROWS)
    is_first, is_last = node == 0, node == last_node

    staged = [
        pltpu.make_async_copy(src, stage.at[i], stage_sem.at[i])
        for i, src in enumerate((key, value, query))
    ]
    gains = [
        pltpu.make_async_copy(src, gain_rows.at[i], gain_sem.at[i])
        for i, src in enumerate((q_gain, k_gain))
    ]
    for copy in staged + gains:
        copy.start()

    barrier = pltpu.get_barrier_semaphore()

    def greet(dev):
        pl.semaphore_signal(barrier, inc=1, device_id=dev, device_id_type=MESH)

    @pl.when(feeds_pair)
    def _():
        for r in range(ROWS):
            for d in range(COLUMNS):
                for c in range(2):
                    if (r, d, c) != (0, 0, 0):
                        greet(device(other_row(r), other_column(d), lax.rem(core + c, 2)))

    greets_ahead = jnp.where(feeds_pair, node != last_node, (node != 0) & (node != last_node))
    greets_behind = jnp.where(feeds_pair, node == 0, node < 2)
    lower = jnp.where(feeds_pair, node != 0, node != 1).astype(jnp.int32) + jnp.where(is_last, 1, 0)
    over_wrap = feeds_pair & is_last
    lower = lower + jnp.where(over_wrap, 1, 0)

    @pl.when(greets_ahead)
    def _():
        greet(device(ahead, x, core))

    @pl.when(greets_behind)
    def _():
        greet(device(behind, x, core))

    @pl.when(is_first & ~feeds_pair)
    def _():
        greet(device(behind, x, FEED_CORE))

    pl.semaphore_wait(barrier, ROWS * COLUMNS - jnp.where(feeds_pair, 1, 0) + lower)

    target = jnp.where(feeds_pair, behind, ahead)
    source = jnp.where(feeds_pair, ahead, behind)

    @pl.when(jnp.where(feeds_pair, node == last_node, node > 1))
    def _():
        pl.semaphore_signal(ready, inc=1, device_id=device(source, x, core), device_id_type=MESH)

    def wait_for_target():
        @pl.when(jnp.where(feeds_pair, node == 0, (node != 0) & (node != last_node)))
        def _():
            pl.semaphore_wait(ready, 1)

    place = pl.ds(pl.multiple_of((x * 2 + core) * tokens, tokens), tokens)

    def feed(i, r, d):
        column = other_column(d)
        dst = (key_raw, value_raw, query_raw.at[z_row])[i].at[place]
        recv = feed_recv.at[i] if i < 2 else feed_recv.at[2 + z_row]
        return pltpu.make_async_remote_copy(
            src_ref=stage.at[i, :, pl.ds(pl.multiple_of(column * lanes, PAD), window)],
            dst_ref=dst,
            send_sem=feed_send.at[i // 2],
            recv_sem=recv,
            device_id=device(other_row(r), column, FEED_CORE),
            device_id_type=MESH,
        )

    def own_feed(i):
        dst = (key_raw, value_raw, query_raw.at[z_row])[i].at[place]
        recv = feed_recv.at[i] if i < 2 else feed_recv.at[2 + z_row]
        src = (key, value, query)[i]
        return pltpu.make_async_copy(
            src.at[:, pl.ds(pl.multiple_of(x * lanes, PAD), window)], dst, recv
        )

    feeds = [(i, r, d) for i in range(3) for r in range(ROWS if i == 2 else 1) for d in (2, 1, 3, 0)]
    for i, r, d in feeds:
        if (r, d) == (0, 2):
            staged[i].wait()
        if (r, d) == (0, 0):

            @pl.when(feeds_pair)
            def _():
                own_feed(i).start()

            @pl.when(core != FEED_CORE)
            def _():
                feed(i, r, d).start()

        else:
            feed(i, r, d).start()

    depth = weight.shape[0]
    mine = whole_weight.at[pl.ds(pl.multiple_of(core * depth, 16), depth)]
    local_weight = pltpu.make_async_copy(weight, mine, weight_sem.at[0])
    sent_weight = pltpu.make_async_remote_copy(
        src_ref=weight,
        dst_ref=mine,
        send_sem=weight_sem.at[1],
        recv_sem=weight_sem.at[2],
        device_id=device(z, x, 1 - core),
        device_id_type=MESH,
    )
    local_weight.start()

    @pl.when(core != FEED_CORE)
    def _():
        sent_weight.start()

    def give_back(r, d, c, h):
        column, a_core = other_column(d), lax.rem(core + c, 2)
        row = lax.rem(z_row + r, ROWS)
        start = row * line + (column * 2 + a_core) * tokens
        return pltpu.make_async_remote_copy(
            src_ref=parts_out.at[h, pl.ds(pl.multiple_of(start, tokens), tokens)],
            dst_ref=parts_in.at[(core * ROWS + z_row) * COLUMNS + x, h],
            send_sem=back_send,
            recv_sem=back_recv,
            device_id=device(other_row(r), column, a_core),
            device_id_type=MESH,
        )

    backs = [(r, d, c) for r in range(ROWS) for d in range(COLUMNS) for c in range(2)]

    def landing(src, p, step, dev, send_sem):
        return pltpu.make_async_remote_copy(
            src_ref=src.at[p],
            dst_ref=ring.at[step, p],
            send_sem=send_sem,
            recv_sem=ring_recv.at[step, p],
            device_id=dev,
            device_id_type=MESH,
        )

    next_node = device(target, x, core)

    def own_on(p):
        return landing(own, p, 0, next_node, ring_send.at[0])

    def own_over_wrap(p):
        return landing(own, p, 0, device(ahead, x, 1 - core), ring_send.at[2])

    def comes_last(h):
        return feeds_pair if h >= HEADS_UP else ~feeds_pair

    def to_pair(ref, p):
        return pltpu.make_async_remote_copy(
            src_ref=ref,
            dst_ref=ref,
            send_sem=pair_send.at[p // pieces],
            recv_sem=pair_recv.at[p],
            device_id=device(z, x, 1 - core),
            device_id_type=MESH,
        )

    scale = float(HD) ** (-0.5) * math.log2(math.e)

    def attend(h, k, v):
        k = jnp.concatenate([k, jnp.zeros((PAD - HD, line), bf16)], axis=0)
        v = jnp.concatenate([v, jnp.ones((PAD - HD, line), bf16)], axis=0)
        scores = jnp.dot(q_heads[h], k, preferred_element_type=f32)
        expd = jnp.exp2(scores * scale).astype(bf16)
        totals[h] += lax.dot_general(expd, v, TN, preferred_element_type=f32)

    totals[...] = jnp.zeros_like(totals)

    @pl.when(feeds_pair)
    def _():
        for i in range(2):
            gains[i].wait()
            gain_pad[...] = jnp.zeros_like(gain_pad)
            gain_pad[:, 0:HD] = jnp.broadcast_to(gain_rows[i], (PAD, HD))
            turned[i, 0:PAD, :] = gain_pad[...].T
        q_column, k_column = turned[0, 0:HD, :], turned[1, 0:HD, :]
        first = x * (group - lanes)

        def head_of(i, h):
            return turned[i, pl.ds(pl.multiple_of(first + h * HD, 32), HD), :]

        def normed(data, gain):
            meansq = jnp.mean(data * data, axis=0, keepdims=True)
            return data * lax.rsqrt(meansq + 1e-06) * gain

        def send_own(kind):
            mine = range(kind * heads, (kind + 1) * heads)

            @pl.when(is_last)
            def _():
                for p in mine:
                    own_over_wrap(p).start()

            @pl.when((node != 0) & (z_row != 1))
            def _():
                for p in mine:
                    own_on(p).start()

            @pl.when(jnp.logical_not(is_last))
            def _():
                for p in mine:
                    to_pair(own.at[p], p).start()

        pltpu.make_async_copy(key_raw, key_raw, feed_recv.at[0]).wait()
        turned[0] = key_raw[...].astype(f32).T
        for h in range(heads):
            own[h] = normed(head_of(0, h), k_column).astype(bf16)
        send_own(0)
        pltpu.make_async_copy(value_raw, value_raw, feed_recv.at[1]).wait()
        turned[1] = value_raw[...].astype(f32).T
        for h in range(heads):
            own[heads + h] = head_of(1, h).astype(bf16)
        send_own(1)

        for r in range(ROWS):
            rows = query_raw.at[r]
            pltpu.make_async_copy(rows, rows, feed_recv.at[2 + r]).wait()
            turned[0] = query_raw[r].astype(f32).T
            for h in range(heads):
                data = normed(head_of(0, h), q_column)
                data = jnp.concatenate([data, jnp.zeros((PAD - HD, line), f32)], axis=0)
                q_heads[h, r * line : (r + 1) * line, :] = data.T.astype(bf16)


        @pl.when((node != 0) & (z_row == 1))
        def _():
            for p in range(pieces):
                own_on(p).start()

        to_pair(q_heads, pieces).start()
        sent_weight.start()
        for h in range(heads):
            attend(h, own[h], own[heads + h])
        wait_for_target()

        @pl.when(node == 0)
        def _():
            for p in range(pieces):
                own_on(p).start()

    @pl.when(core != FEED_CORE)
    def _():
        for copy in gains:
            copy.wait()
        wait_for_target()

        @pl.when(jnp.logical_not(is_last))
        def _():
            for p in range(pieces):
                to_pair(own.at[p], p).wait_recv()
                own_on(p).start()

        to_pair(q_heads, pieces).wait_recv()

    lane = lax.broadcasted_iota(jnp.int32, (ROWS * line, PAD), 1)

    def arrives(step, p):
        landing(own, p, step, next_node, ring_send.at[0]).wait_recv()

    def chunk(step, carry):
        for p in range(pieces):
            arrives(step, p)

            @pl.when(step < steps - 2)
            def _():
                landing(ring.at[step], p, step + 1, next_node, ring_send.at[0]).start()

            @pl.when((step == steps - 2) & comes_last(p % heads))
            def _():
                landing(ring.at[step], p, step + 1, next_node, ring_send.at[1]).start()

            if p >= heads:
                attend(p - heads, ring[step, p - heads], ring[step, p])
        return carry

    lax.fori_loop(0, steps - 1, chunk, 0)

    def give(h):
        total = totals[h]
        high = total.astype(bf16)
        low = (total - high.astype(f32)).astype(bf16)
        parts_out[h] = jnp.where(lane >= HD + 16, low, high)
        for r, d, c in backs:
            if (r, d, c) != (0, 0, 0):
                give_back(r, d, c, h).start()

    for h in range(heads):

        @pl.when(jnp.logical_not(comes_last(h)))
        def _():
            give(h)

    for h in range(heads):

        @pl.when(comes_last(h))
        def _():
            arrives(steps - 1, h)
            arrives(steps - 1, heads + h)
            attend(h, ring[steps - 1, h], ring[steps - 1, heads + h])
            give(h)

    own_start = z_row * line + (x * 2 + core) * tokens
    for h in range(heads):
        parts_in[(core * ROWS + z_row) * COLUMNS + x, h] = parts_out[
            h, pl.ds(pl.multiple_of(own_start, tokens), tokens)
        ]

    def left(ref, sem):
        pltpu.make_async_copy(ref, ref, sem).wait()

    @pl.when(feeds_pair)
    def _():
        ways = COLUMNS - 1
        left(key_raw.at[0 : 2 * ways * tokens], feed_send.at[0])
        left(key_raw.at[0 : (ROWS * COLUMNS - 1) * tokens], feed_send.at[1])
        left(q_heads, pair_send.at[1])
        left(ring.at[0 : nodes - AHEAD - 1], ring_send.at[0])
        left(ring.at[0, 0 : 2 * (heads - HEADS_UP)], ring_send.at[1])

        @pl.when(is_last)
        def _():
            left(own, ring_send.at[2])

        @pl.when(jnp.logical_not(is_last))
        def _():
            left(own, pair_send.at[0])

    @pl.when(core != FEED_CORE)
    def _():
        left(key_raw.at[0 : 2 * COLUMNS * tokens], feed_send.at[0])
        left(key_raw.at[0 : ROWS * COLUMNS * tokens], feed_send.at[1])
        left(ring.at[0, 0 : 2 * HEADS_UP], ring_send.at[1])

        @pl.when(is_last)
        def _():
            left(ring.at[0 : AHEAD - 2], ring_send.at[0])

        @pl.when(jnp.logical_not(is_last))
        def _():
            left(ring.at[0 : AHEAD - 1], ring_send.at[0])

    left(parts_out.at[:, 0 : (len(backs) - 1) * tokens], back_send)

    local_weight.wait()
    sent_weight.wait()
    attn = []
    others = parts_in.at[0 : len(backs) - 1]
    pltpu.make_async_copy(others, others, back_recv).wait()
    for d in range(COLUMNS):
        for h in range(heads):
            part = sum(
                parts_in[i * COLUMNS + d, h].astype(f32)
                for i in range(2 * ROWS)
            )
            total_weight = part[:, HD : HD + 1] + part[:, HD + 16 : HD + 17]
            attn.append((part[:, 0:HD] / total_weight).astype(bf16))
    attn = jnp.concatenate(attn, axis=1)
    mixed[...] = jnp.dot(attn, whole_weight[...], preferred_element_type=f32).astype(bf16)


def on_device(lines, query, key, value, q_gain, k_gain, out_weight):
    tokens, width = query.shape
    heads = width // HD // COLUMNS
    nodes = lines // ROWS
    pieces = 2 * heads
    most = max(AHEAD, nodes - AHEAD)
    line = 2 * COLUMNS * tokens
    window = 3 * PAD
    f32, bf16 = jnp.float32, jnp.bfloat16
    hbm = pl.BlockSpec(memory_space=pl.ANY)
    vmem = pl.BlockSpec(memory_space=pltpu.VMEM)
    dma = pltpu.SemaphoreType.DMA
    return pl.pallas_call(
        functools.partial(kernel, nodes, heads),
        out_shape=pltpu.VMEM((tokens, out_weight.shape[1]), bf16),
        in_specs=[hbm] * 6,
        out_specs=vmem,
        scratch_shapes=[
            pltpu.VMEM((3, tokens, width), bf16),
            pltpu.VMEM((line, window), bf16),
            pltpu.VMEM((line, window), bf16),
            pltpu.VMEM((ROWS, line, window), bf16),
            pltpu.VMEM((2, window, line), f32),
            pltpu.VMEM((2, 1, HD), f32),
            pltpu.VMEM((PAD, PAD), f32),
            pltpu.VMEM((pieces, HD, line), bf16),
            pltpu.VMEM((most, pieces, HD, line), bf16),
            pltpu.VMEM((heads, ROWS * line, PAD), bf16),
            pltpu.VMEM((heads, ROWS * line, PAD), f32),
            pltpu.VMEM((heads, ROWS * line, PAD), bf16),
            pltpu.VMEM((2 * ROWS * COLUMNS, heads, tokens, PAD), bf16),
            pltpu.VMEM((2 * out_weight.shape[0], out_weight.shape[1]), bf16),
            dma((3,)),
            dma((2,)),
            dma((2,)),
            dma((2 + ROWS,)),
            dma((3,)),
            dma((most, pieces)),
            dma,
            dma,
            dma((3,)),
            dma((2,)),
            dma((pieces + 1,)),
            pltpu.SemaphoreType.REGULAR,
        ],
        compiler_params=pltpu.CompilerParams(collective_id=0, has_side_effects=True),
        name="attention",
    )(query, key, value, q_gain.reshape(1, HD), k_gain.reshape(1, HD), out_weight)


def solution(mesh):
    tokens = P(("grp", "blk", "uly"), None)
    return jax.shard_map(
        functools.partial(on_device, mesh.shape["blk"] // COLUMNS),
        mesh=mesh,
        in_specs=(tokens, tokens, tokens, P(), P(), P("uly", None)),
        out_specs=tokens,
        check_vma=False,
    )
```

```python
import functools
import math

import jax
import jax.numpy as jnp
from jax import lax
from jax.experimental import pallas as pl
from jax.experimental.pallas import tpu as pltpu
from jax.sharding import PartitionSpec as P

HD = 96
PAD = 128
COLUMNS = 4
ROWS = 2
FEED_CORE = 1
AHEAD = 6
HEADS_UP = 3
MESH = pl.DeviceIdType.MESH
TN = (((1,), (1,)), ((), ()))


def kernel(
    nodes,
    heads,
    query,
    key,
    value,
    q_gain,
    k_gain,
    weight,
    mixed,
    stage,
    key_raw,
    value_raw,
    query_raw,
    turned,
    gain_rows,
    gain_pad,
    own,
    ring,
    q_heads,
    totals,
    parts_out,
    parts_in,
    whole_weight,
    stage_sem,
    gain_sem,
    feed_send,
    feed_recv,
    ring_send,
    ring_recv,
    back_send,
    back_recv,
    weight_sem,
    pair_send,
    pair_recv,
    ready,
    row_ready,
):
    f32, bf16 = jnp.float32, jnp.bfloat16
    block = lax.axis_index("blk")
    core = lax.axis_index("uly")
    z, x = lax.div(block, COLUMNS), lax.rem(block, COLUMNS)
    z_block, z_row = lax.div(z, ROWS), lax.rem(z, ROWS)
    feeds_pair = core == FEED_CORE
    tokens = query.shape[0]
    window = 3 * PAD
    lanes = 2 * PAD
    group = heads * HD
    line = 2 * COLUMNS * tokens
    pieces = 2 * heads
    split = HEADS_UP < heads
    steps = jnp.where(feeds_pair, nodes - AHEAD - (0 if split else 1), AHEAD)

    def device(row, column, a_core):
        return {"blk": row * COLUMNS + column, "uly": a_core}

    def other_row(r):
        return z_block * ROWS + lax.rem(z_row + r, ROWS)

    def other_column(d):
        return lax.rem(x + d, COLUMNS)

    node, last_node = z_block, nodes - 1
    ahead = lax.rem(z + ROWS, nodes * ROWS)
    behind = lax.rem(z + last_node * ROWS, nodes * ROWS)
    is_first, is_last = node == 0, node == last_node

    staged = [
        pltpu.make_async_copy(src, stage.at[i], stage_sem.at[i])
        for i, src in enumerate((key, value, query))
    ]
    gains = [
        pltpu.make_async_copy(src, gain_rows.at[i], gain_sem.at[i])
        for i, src in enumerate((q_gain, k_gain))
    ]
    for copy in staged + gains:
        copy.start()

    barrier = pltpu.get_barrier_semaphore()

    def greet(dev):
        pl.semaphore_signal(barrier, inc=1, device_id=dev, device_id_type=MESH)

    first_row = z_row == 0

    @pl.when(feeds_pair)
    def _():
        for d in range(COLUMNS):
            for c in range(2):
                if (d, c) != (0, 0):
                    greet(device(z, other_column(d), lax.rem(core + c, 2)))

    @pl.when(first_row & (feeds_pair | (node != 0)))
    def _():
        for d in range(COLUMNS):
            greet(device(z + 1, other_column(d), FEED_CORE))

    @pl.when(first_row & feeds_pair)
    def _():
        for d in range(COLUMNS):
            greet(device(z + 1, other_column(d), 1 - FEED_CORE))

    before = jnp.where(
        feeds_pair,
        jnp.where(first_row, COLUMNS - 1, jnp.where(is_first, 2, 3) * COLUMNS - 1),
        jnp.where(first_row, COLUMNS, 2 * COLUMNS),
    )

    greets_ahead = jnp.where(feeds_pair, node != last_node, (node != 0) & (node != last_node))
    greets_behind = jnp.where(feeds_pair, node == 0, node < 2)
    lower = jnp.where(feeds_pair, node != 0, node != 1).astype(jnp.int32) + jnp.where(is_last, 1, 0)
    over_wrap = feeds_pair & is_last
    lower = lower + jnp.where(over_wrap, 1, 0)

    @pl.when(greets_ahead)
    def _():
        greet(device(ahead, x, core))

    @pl.when(greets_behind)
    def _():
        greet(device(behind, x, core))

    @pl.when(is_first & ~feeds_pair)
    def _():
        greet(device(behind, x, FEED_CORE))

    pl.semaphore_wait(barrier, before + lower)

    def tell(row, column, a_core, times):
        pl.semaphore_signal(
            row_ready, inc=times, device_id=device(row, column, a_core), device_id_type=MESH
        )

    for c in range(2):

        @pl.when(feeds_pair & ~first_row & ((node != 0) | (c == FEED_CORE)))
        def _():
            for d in range(COLUMNS):
                tell(z - 1, other_column(d), c, 1)

    target = jnp.where(feeds_pair, behind, ahead)
    source = jnp.where(feeds_pair, ahead, behind)

    @pl.when(jnp.where(feeds_pair, node == last_node, node > 1))
    def _():
        pl.semaphore_signal(ready, inc=1, device_id=device(source, x, core), device_id_type=MESH)

    def wait_for_target():
        @pl.when(jnp.where(feeds_pair, node == 0, (node != 0) & (node != last_node)))
        def _():
            pl.semaphore_wait(ready, 1)

    place = pl.ds(pl.multiple_of((x * 2 + core) * tokens, tokens), tokens)

    def feed(i, r, d):
        column = other_column(d)
        dst = (key_raw, value_raw, query_raw.at[z_row])[i].at[place]
        recv = feed_recv.at[i] if i < 2 else feed_recv.at[2 + z_row]
        return pltpu.make_async_remote_copy(
            src_ref=stage.at[i, :, pl.ds(pl.multiple_of(column * lanes, PAD), window)],
            dst_ref=dst,
            send_sem=feed_send.at[i // 2],
            recv_sem=recv,
            device_id=device(other_row(r), column, FEED_CORE),
            device_id_type=MESH,
        )

    def own_feed(i):
        dst = (key_raw, value_raw, query_raw.at[z_row])[i].at[place]
        recv = feed_recv.at[i] if i < 2 else feed_recv.at[2 + z_row]
        src = (key, value, query)[i]
        return pltpu.make_async_copy(
            src.at[:, pl.ds(pl.multiple_of(x * lanes, PAD), window)], dst, recv
        )

    feeds = [(i, r, d) for i in range(3) for r in range(ROWS if i == 2 else 1) for d in (2, 1, 3, 0)]
    for i, r, d in feeds:
        if (r, d) == (0, 2):
            staged[i].wait()
        if (r, d) == (1, 2):

            @pl.when(first_row)
            def _():
                pl.semaphore_wait(row_ready, COLUMNS)

        if (r, d) == (0, 0):

            @pl.when(feeds_pair)
            def _():
                own_feed(i).start()

            @pl.when(core != FEED_CORE)
            def _():
                feed(i, r, d).start()

        else:
            feed(i, r, d).start()

    depth = weight.shape[0]
    mine = whole_weight.at[pl.ds(pl.multiple_of(core * depth, 16), depth)]
    local_weight = pltpu.make_async_copy(weight, mine, weight_sem.at[0])
    sent_weight = pltpu.make_async_remote_copy(
        src_ref=weight,
        dst_ref=mine,
        send_sem=weight_sem.at[1],
        recv_sem=weight_sem.at[2],
        device_id=device(z, x, 1 - core),
        device_id_type=MESH,
    )
    local_weight.start()

    @pl.when(core != FEED_CORE)
    def _():
        sent_weight.start()

    def give_back(r, d, c, h):
        column, a_core = other_column(d), lax.rem(core + c, 2)
        row = lax.rem(z_row + r, ROWS)
        start = row * line + (column * 2 + a_core) * tokens
        return pltpu.make_async_remote_copy(
            src_ref=parts_out.at[h, pl.ds(pl.multiple_of(start, tokens), tokens)],
            dst_ref=parts_in.at[(core * ROWS + z_row) * COLUMNS + x, h],
            send_sem=back_send,
            recv_sem=back_recv,
            device_id=device(other_row(r), column, a_core),
            device_id_type=MESH,
        )

    backs = [(r, d, c) for r in range(ROWS) for d in range(COLUMNS) for c in range(2)]

    def landing(src, p, step, dev, send_sem):
        return pltpu.make_async_remote_copy(
            src_ref=src.at[p],
            dst_ref=ring.at[step, p],
            send_sem=send_sem,
            recv_sem=ring_recv.at[step, p],
            device_id=dev,
            device_id_type=MESH,
        )

    next_node = device(target, x, core)

    def own_on(p):
        return landing(own, p, 0, next_node, ring_send.at[0])

    def own_over_wrap(p):
        return landing(own, p, 0, device(ahead, x, 1 - core), ring_send.at[2])

    def comes_last(h):
        return feeds_pair | ~feeds_pair if not split else feeds_pair if h >= HEADS_UP else ~feeds_pair

    def to_pair(ref, p):
        return pltpu.make_async_remote_copy(
            src_ref=ref,
            dst_ref=ref,
            send_sem=pair_send.at[p // pieces],
            recv_sem=pair_recv.at[p],
            device_id=device(z, x, 1 - core),
            device_id_type=MESH,
        )

    scale = float(HD) ** (-0.5) * math.log2(math.e)

    def attend(h, k, v):
        k = jnp.concatenate([k, jnp.zeros((PAD - HD, line), bf16)], axis=0)
        v = jnp.concatenate([v, jnp.ones((PAD - HD, line), bf16)], axis=0)
        scores = jnp.dot(q_heads[h], k, preferred_element_type=f32)
        expd = jnp.exp2(scores * scale).astype(bf16)
        totals[h] += lax.dot_general(expd, v, TN, preferred_element_type=f32)

    totals[...] = jnp.zeros_like(totals)

    @pl.when(feeds_pair)
    def _():
        for i in range(2):
            gains[i].wait()
            gain_pad[...] = jnp.zeros_like(gain_pad)
            gain_pad[:, 0:HD] = jnp.broadcast_to(gain_rows[i], (PAD, HD))
            turned[i, 0:PAD, :] = gain_pad[...].T
        q_column, k_column = turned[0, 0:HD, :], turned[1, 0:HD, :]
        first = x * (group - lanes)

        def head_of(i, h):
            return turned[i, pl.ds(pl.multiple_of(first + h * HD, 32), HD), :]

        def normed(data, gain):
            meansq = jnp.mean(data * data, axis=0, keepdims=True)
            return data * lax.rsqrt(meansq + 1e-06) * gain

        def send_own(kind):
            mine = range(kind * heads, (kind + 1) * heads)

            @pl.when(is_last)
            def _():
                for p in mine:
                    own_over_wrap(p).start()

            @pl.when((node != 0) & first_row)
            def _():
                for p in mine:
                    own_on(p).start()

            if kind == 1:

                @pl.when((node != 0) & ~first_row)
                def _():
                    for p in range(pieces):
                        own_on(p).start()

            @pl.when(jnp.logical_not(is_last))
            def _():
                for p in mine:
                    to_pair(own.at[p], p).start()

        pltpu.make_async_copy(key_raw, key_raw, feed_recv.at[0]).wait()

        @pl.when(is_first & first_row)
        def _():
            tell(z, x, 1 - FEED_CORE, COLUMNS)

        turned[0] = key_raw[...].astype(f32).T
        for h in range(heads):
            own[h] = normed(head_of(0, h), k_column).astype(bf16)
        send_own(0)
        pltpu.make_async_copy(value_raw, value_raw, feed_recv.at[1]).wait()
        turned[1] = value_raw[...].astype(f32).T
        for h in range(heads):
            own[heads + h] = head_of(1, h).astype(bf16)
        send_own(1)

        for r in range(ROWS):
            rows = query_raw.at[r]
            pltpu.make_async_copy(rows, rows, feed_recv.at[2 + r]).wait()
            turned[0] = query_raw[r].astype(f32).T
            for h in range(heads):
                data = normed(head_of(0, h), q_column)
                data = jnp.concatenate([data, jnp.zeros((PAD - HD, line), f32)], axis=0)
                q_heads[h, r * line : (r + 1) * line, :] = data.T.astype(bf16)

        to_pair(q_heads, pieces).start()
        sent_weight.start()
        for h in range(heads):
            attend(h, own[h], own[heads + h])
        wait_for_target()

        @pl.when(node == 0)
        def _():
            for p in range(pieces):
                own_on(p).start()

    @pl.when(core != FEED_CORE)
    def _():
        for copy in gains:
            copy.wait()
        wait_for_target()

        @pl.when(jnp.logical_not(is_last))
        def _():
            for p in range(pieces):
                to_pair(own.at[p], p).wait_recv()
                own_on(p).start()

        to_pair(q_heads, pieces).wait_recv()

    lane = lax.broadcasted_iota(jnp.int32, (ROWS * line, PAD), 1)

    def arrives(step, p):
        landing(own, p, step, next_node, ring_send.at[0]).wait_recv()

    def chunk(step, carry):
        for p in range(pieces):
            arrives(step, p)

            @pl.when(step < steps - 2)
            def _():
                landing(ring.at[step], p, step + 1, next_node, ring_send.at[0]).start()

            @pl.when((step == steps - 2) & comes_last(p % heads))
            def _():
                landing(ring.at[step], p, step + 1, next_node, ring_send.at[1]).start()

            if p >= heads:
                attend(p - heads, ring[step, p - heads], ring[step, p])
        return carry

    lax.fori_loop(0, steps - 1, chunk, 0)

    def give(h):
        total = totals[h]
        high = total.astype(bf16)
        low = (total - high.astype(f32)).astype(bf16)
        parts_out[h] = jnp.where(lane >= HD + 16, low, high)
        for r, d, c in backs:
            if (r, d, c) != (0, 0, 0):
                give_back(r, d, c, h).start()

    for h in range(heads):

        @pl.when(jnp.logical_not(comes_last(h)))
        def _():
            give(h)

    for h in range(heads):

        @pl.when(comes_last(h))
        def _():
            arrives(steps - 1, h)
            arrives(steps - 1, heads + h)
            attend(h, ring[steps - 1, h], ring[steps - 1, heads + h])
            give(h)

    own_start = z_row * line + (x * 2 + core) * tokens
    for h in range(heads):
        parts_in[(core * ROWS + z_row) * COLUMNS + x, h] = parts_out[
            h, pl.ds(pl.multiple_of(own_start, tokens), tokens)
        ]

    def left(ref, sem):
        pltpu.make_async_copy(ref, ref, sem).wait()

    @pl.when(feeds_pair)
    def _():
        ways = COLUMNS - 1
        left(key_raw.at[0 : 2 * ways * tokens], feed_send.at[0])
        left(key_raw.at[0 : (ROWS * COLUMNS - 1) * tokens], feed_send.at[1])
        left(q_heads, pair_send.at[1])
        left(ring.at[0 : nodes - AHEAD - (1 if split else 2)], ring_send.at[0])
        left(ring.at[0, 0 : 2 * (heads - HEADS_UP) if split else pieces], ring_send.at[1])

        @pl.when(is_last)
        def _():
            left(own, ring_send.at[2])

        @pl.when(jnp.logical_not(is_last))
        def _():
            left(own, pair_send.at[0])

    @pl.when(core != FEED_CORE)
    def _():
        left(key_raw.at[0 : 2 * COLUMNS * tokens], feed_send.at[0])
        left(key_raw.at[0 : ROWS * COLUMNS * tokens], feed_send.at[1])
        left(ring.at[0, 0 : 2 * HEADS_UP], ring_send.at[1])

        @pl.when(is_last)
        def _():
            left(ring.at[0 : AHEAD - 2], ring_send.at[0])

        @pl.when(jnp.logical_not(is_last))
        def _():
            left(ring.at[0 : AHEAD - 1], ring_send.at[0])

    left(parts_out.at[:, 0 : (len(backs) - 1) * tokens], back_send)

    local_weight.wait()
    sent_weight.wait()
    attn = []
    others = parts_in.at[0 : len(backs) - 1]
    pltpu.make_async_copy(others, others, back_recv).wait()
    for d in range(COLUMNS):
        for h in range(heads):
            part = sum(
                parts_in[i * COLUMNS + d, h].astype(f32)
                for i in range(2 * ROWS)
            )
            total_weight = part[:, HD : HD + 1] + part[:, HD + 16 : HD + 17]
            attn.append((part[:, 0:HD] / total_weight).astype(bf16))
    attn = jnp.concatenate(attn, axis=1)
    mixed[...] = jnp.dot(attn, whole_weight[...], preferred_element_type=f32).astype(bf16)


def on_device(lines, query, key, value, q_gain, k_gain, out_weight):
    tokens, width = query.shape
    heads = width // HD // COLUMNS
    nodes = lines // ROWS
    pieces = 2 * heads
    most = max(AHEAD, nodes - AHEAD)
    line = 2 * COLUMNS * tokens
    window = 3 * PAD
    f32, bf16 = jnp.float32, jnp.bfloat16
    hbm = pl.BlockSpec(memory_space=pl.ANY)
    vmem = pl.BlockSpec(memory_space=pltpu.VMEM)
    dma = pltpu.SemaphoreType.DMA
    return pl.pallas_call(
        functools.partial(kernel, nodes, heads),
        out_shape=pltpu.VMEM((tokens, out_weight.shape[1]), bf16),
        in_specs=[hbm] * 6,
        out_specs=vmem,
        scratch_shapes=[
            pltpu.VMEM((3, tokens, width), bf16),
            pltpu.VMEM((line, window), bf16),
            pltpu.VMEM((line, window), bf16),
            pltpu.VMEM((ROWS, line, window), bf16),
            pltpu.VMEM((2, window, line), f32),
            pltpu.VMEM((2, 1, HD), f32),
            pltpu.VMEM((PAD, PAD), f32),
            pltpu.VMEM((pieces, HD, line), bf16),
            pltpu.VMEM((most, pieces, HD, line), bf16),
            pltpu.VMEM((heads, ROWS * line, PAD), bf16),
            pltpu.VMEM((heads, ROWS * line, PAD), f32),
            pltpu.VMEM((heads, ROWS * line, PAD), bf16),
            pltpu.VMEM((2 * ROWS * COLUMNS, heads, tokens, PAD), bf16),
            pltpu.VMEM((2 * out_weight.shape[0], out_weight.shape[1]), bf16),
            dma((3,)),
            dma((2,)),
            dma((2,)),
            dma((2 + ROWS,)),
            dma((3,)),
            dma((most, pieces)),
            dma,
            dma,
            dma((3,)),
            dma((2,)),
            dma((pieces + 1,)),
            pltpu.SemaphoreType.REGULAR,
            pltpu.SemaphoreType.REGULAR,
        ],
        compiler_params=pltpu.CompilerParams(collective_id=0, has_side_effects=True),
        name="attention",
    )(query, key, value, q_gain.reshape(1, HD), k_gain.reshape(1, HD), out_weight)


def solution(mesh):
    tokens = P(("grp", "blk", "uly"), None)
    return jax.shard_map(
        functools.partial(on_device, mesh.shape["blk"] // COLUMNS),
        mesh=mesh,
        in_specs=(tokens, tokens, tokens, P(), P(), P("uly", None)),
        out_specs=tokens,
        check_vma=False,
    )
```

```python
import functools
import math

import jax
import jax.numpy as jnp
from jax import lax
from jax.experimental import pallas as pl
from jax.experimental.pallas import tpu as pltpu
from jax.sharding import PartitionSpec as P

HD = 96
PAD = 128
COLUMNS = 4
ROWS = 2
FEED_CORE = 1
AHEAD = 6
HEADS_UP = 3
MESH = pl.DeviceIdType.MESH
TN = (((1,), (1,)), ((), ()))


def kernel(
    nodes,
    heads,
    query,
    key,
    value,
    q_gain,
    k_gain,
    weight,
    mixed,
    stage,
    key_raw,
    value_raw,
    query_raw,
    turned,
    gain_rows,
    gain_pad,
    own,
    ring,
    q_heads,
    totals,
    parts_out,
    parts_in,
    whole_weight,
    stage_sem,
    gain_sem,
    feed_send,
    feed_recv,
    ring_send,
    ring_recv,
    back_send,
    back_recv,
    weight_sem,
    pair_send,
    pair_recv,
    ready,
    row_ready,
):
    f32, bf16 = jnp.float32, jnp.bfloat16
    block = lax.axis_index("blk")
    core = lax.axis_index("uly")
    z, x = lax.div(block, COLUMNS), lax.rem(block, COLUMNS)
    z_block, z_row = lax.div(z, ROWS), lax.rem(z, ROWS)
    feeds_pair = core == FEED_CORE
    tokens = query.shape[0]
    window = 3 * PAD
    lanes = 2 * PAD
    group = heads * HD
    line = 2 * COLUMNS * tokens
    pieces = 2 * heads
    split = HEADS_UP < heads
    steps = jnp.where(feeds_pair, nodes - AHEAD - (0 if split else 1), AHEAD)

    def device(row, column, a_core):
        return {"blk": row * COLUMNS + column, "uly": a_core}

    def other_row(r):
        return z_block * ROWS + lax.rem(z_row + r, ROWS)

    def other_column(d):
        return lax.rem(x + d, COLUMNS)

    node, last_node = z_block, nodes - 1
    ahead = lax.rem(z + ROWS, nodes * ROWS)
    behind = lax.rem(z + last_node * ROWS, nodes * ROWS)
    is_first, is_last = node == 0, node == last_node

    staged = [
        pltpu.make_async_copy(src, stage.at[i], stage_sem.at[i])
        for i, src in enumerate((key, value, query))
    ]
    gains = [
        pltpu.make_async_copy(src, gain_rows.at[i], gain_sem.at[i])
        for i, src in enumerate((q_gain, k_gain))
    ]
    for copy in staged + gains:
        copy.start()

    barrier = pltpu.get_barrier_semaphore()

    def greet(dev):
        pl.semaphore_signal(barrier, inc=1, device_id=dev, device_id_type=MESH)

    first_row = z_row == 0

    @pl.when(feeds_pair)
    def _():
        for d in range(COLUMNS):
            for c in range(2):
                if (d, c) != (0, 0):
                    greet(device(z, other_column(d), lax.rem(core + c, 2)))

    @pl.when(first_row & (feeds_pair | (node != 0)))
    def _():
        for d in range(COLUMNS):
            greet(device(z + 1, other_column(d), FEED_CORE))

    @pl.when(first_row & feeds_pair)
    def _():
        for d in range(COLUMNS):
            greet(device(z + 1, other_column(d), 1 - FEED_CORE))

    before = jnp.where(
        feeds_pair,
        jnp.where(first_row, COLUMNS - 1, jnp.where(is_first, 2, 3) * COLUMNS - 1),
        jnp.where(first_row, COLUMNS, 2 * COLUMNS),
    )

    greets_ahead = jnp.where(feeds_pair, node != last_node, (node != 0) & (node != last_node))
    greets_behind = jnp.where(feeds_pair, node == 0, node < 2)
    lower = jnp.where(feeds_pair, node != 0, node != 1).astype(jnp.int32) + jnp.where(is_last, 1, 0)
    over_wrap = feeds_pair & is_last
    lower = lower + jnp.where(over_wrap, 1, 0)

    @pl.when(greets_ahead)
    def _():
        greet(device(ahead, x, core))

    @pl.when(greets_behind)
    def _():
        greet(device(behind, x, core))

    @pl.when(is_first & ~feeds_pair)
    def _():
        greet(device(behind, x, FEED_CORE))

    pl.semaphore_wait(barrier, before + lower)

    def tell(row, column, a_core, times):
        pl.semaphore_signal(
            row_ready, inc=times, device_id=device(row, column, a_core), device_id_type=MESH
        )

    for c in range(2):

        @pl.when(feeds_pair & ~first_row & ((node != 0) | (c == FEED_CORE)))
        def _():
            for d in range(COLUMNS):
                tell(z - 1, other_column(d), c, 1)

    target = jnp.where(feeds_pair, behind, ahead)
    source = jnp.where(feeds_pair, ahead, behind)

    @pl.when(jnp.where(feeds_pair, node == last_node, node > 1))
    def _():
        pl.semaphore_signal(ready, inc=1, device_id=device(source, x, core), device_id_type=MESH)

    def wait_for_target():
        @pl.when(jnp.where(feeds_pair, node == 0, (node != 0) & (node != last_node)))
        def _():
            pl.semaphore_wait(ready, 1)

    place = pl.ds(pl.multiple_of((x * 2 + core) * tokens, tokens), tokens)

    def feed(i, r, d):
        column = other_column(d)
        dst = (key_raw, value_raw, query_raw.at[z_row])[i].at[place]
        recv = feed_recv.at[i] if i < 2 else feed_recv.at[2 + z_row]
        return pltpu.make_async_remote_copy(
            src_ref=stage.at[i, :, pl.ds(pl.multiple_of(column * lanes, PAD), window)],
            dst_ref=dst,
            send_sem=feed_send.at[i // 2],
            recv_sem=recv,
            device_id=device(other_row(r), column, FEED_CORE),
            device_id_type=MESH,
        )

    def own_feed(i):
        dst = (key_raw, value_raw, query_raw.at[z_row])[i].at[place]
        recv = feed_recv.at[i] if i < 2 else feed_recv.at[2 + z_row]
        src = (key, value, query)[i]
        return pltpu.make_async_copy(
            src.at[:, pl.ds(pl.multiple_of(x * lanes, PAD), window)], dst, recv
        )

    feeds = [(i, r, d) for i in range(3) for r in range(ROWS if i == 2 else 1) for d in (2, 1, 3, 0)]
    for i, r, d in feeds:
        if (r, d) == (0, 2):
            staged[i].wait()
        if (r, d) == (1, 2):

            @pl.when(first_row)
            def _():
                pl.semaphore_wait(row_ready, COLUMNS)

        if (r, d) == (0, 0):

            @pl.when(feeds_pair)
            def _():
                own_feed(i).start()

            @pl.when(core != FEED_CORE)
            def _():
                feed(i, r, d).start()

        else:
            feed(i, r, d).start()

    depth = weight.shape[0]
    mine = whole_weight.at[pl.ds(pl.multiple_of(core * depth, 16), depth)]
    local_weight = pltpu.make_async_copy(weight, mine, weight_sem.at[0])
    sent_weight = pltpu.make_async_remote_copy(
        src_ref=weight,
        dst_ref=mine,
        send_sem=weight_sem.at[1],
        recv_sem=weight_sem.at[2],
        device_id=device(z, x, 1 - core),
        device_id_type=MESH,
    )
    local_weight.start()

    @pl.when(core != FEED_CORE)
    def _():
        sent_weight.start()

    def give_back(r, d, c, h):
        column, a_core = other_column(d), lax.rem(core + c, 2)
        row = lax.rem(z_row + r, ROWS)
        start = row * line + (column * 2 + a_core) * tokens
        return pltpu.make_async_remote_copy(
            src_ref=parts_out.at[h, pl.ds(pl.multiple_of(start, tokens), tokens)],
            dst_ref=parts_in.at[(core * ROWS + z_row) * COLUMNS + x, h],
            send_sem=back_send,
            recv_sem=back_recv,
            device_id=device(other_row(r), column, a_core),
            device_id_type=MESH,
        )

    backs = [(r, d, c) for r in (1, 0) for d in (2, 1, 3, 0) for c in range(2)]

    def landing(src, p, step, dev, send_sem):
        return pltpu.make_async_remote_copy(
            src_ref=src.at[p],
            dst_ref=ring.at[step, p],
            send_sem=send_sem,
            recv_sem=ring_recv.at[step, p],
            device_id=dev,
            device_id_type=MESH,
        )

    next_node = device(target, x, core)

    def own_on(p):
        return landing(own, p, 0, next_node, ring_send.at[0])

    def own_over_wrap(p):
        return landing(own, p, 0, device(ahead, x, 1 - core), ring_send.at[2])

    def comes_last(h):
        return feeds_pair | ~feeds_pair if not split else feeds_pair if h >= HEADS_UP else ~feeds_pair

    def to_pair(ref, p):
        return pltpu.make_async_remote_copy(
            src_ref=ref,
            dst_ref=ref,
            send_sem=pair_send.at[p // pieces],
            recv_sem=pair_recv.at[p],
            device_id=device(z, x, 1 - core),
            device_id_type=MESH,
        )

    scale = float(HD) ** (-0.5) * math.log2(math.e)

    def attend(h, k, v):
        k = jnp.concatenate([k, jnp.zeros((PAD - HD, line), bf16)], axis=0)
        v = jnp.concatenate([v, jnp.ones((PAD - HD, line), bf16)], axis=0)
        scores = jnp.dot(q_heads[h], k, preferred_element_type=f32)
        expd = jnp.exp2(scores * scale).astype(bf16)
        totals[h] += lax.dot_general(expd, v, TN, preferred_element_type=f32)

    totals[...] = jnp.zeros_like(totals)

    @pl.when(feeds_pair)
    def _():
        for i in range(2):
            gains[i].wait()
            gain_pad[...] = jnp.zeros_like(gain_pad)
            gain_pad[:, 0:HD] = jnp.broadcast_to(gain_rows[i], (PAD, HD))
            turned[i, 0:PAD, :] = gain_pad[...].T
        q_column, k_column = turned[0, 0:HD, :], turned[1, 0:HD, :]
        first = x * (group - lanes)

        def head_of(i, h):
            return turned[i, pl.ds(pl.multiple_of(first + h * HD, 32), HD), :]

        def normed(data, gain):
            meansq = jnp.mean(data * data, axis=0, keepdims=True)
            return data * lax.rsqrt(meansq + 1e-06) * gain

        def send_own(kind):
            mine = range(kind * heads, (kind + 1) * heads)

            @pl.when(is_last)
            def _():
                for p in mine:
                    own_over_wrap(p).start()

            @pl.when((node != 0) & first_row)
            def _():
                for p in mine:
                    own_on(p).start()

            if kind == 1:

                @pl.when((node != 0) & ~first_row)
                def _():
                    for p in range(pieces):
                        own_on(p).start()

            @pl.when(jnp.logical_not(is_last))
            def _():
                for p in mine:
                    to_pair(own.at[p], p).start()

        pltpu.make_async_copy(key_raw, key_raw, feed_recv.at[0]).wait()

        @pl.when(is_first & first_row)
        def _():
            tell(z, x, 1 - FEED_CORE, COLUMNS)

        turned[0] = key_raw[...].astype(f32).T
        for h in range(heads):
            own[h] = normed(head_of(0, h), k_column).astype(bf16)
        send_own(0)
        pltpu.make_async_copy(value_raw, value_raw, feed_recv.at[1]).wait()
        turned[1] = value_raw[...].astype(f32).T
        for h in range(heads):
            own[heads + h] = head_of(1, h).astype(bf16)
        send_own(1)

        for r in range(ROWS):
            rows = query_raw.at[r]
            pltpu.make_async_copy(rows, rows, feed_recv.at[2 + r]).wait()
            turned[0] = query_raw[r].astype(f32).T
            for h in range(heads):
                data = normed(head_of(0, h), q_column)
                data = jnp.concatenate([data, jnp.zeros((PAD - HD, line), f32)], axis=0)
                q_heads[h, r * line : (r + 1) * line, :] = data.T.astype(bf16)

        to_pair(q_heads, pieces).start()
        sent_weight.start()
        for h in range(heads):
            attend(h, own[h], own[heads + h])
        wait_for_target()

        @pl.when(node == 0)
        def _():
            for p in range(pieces):
                own_on(p).start()

    @pl.when(core != FEED_CORE)
    def _():
        for copy in gains:
            copy.wait()
        wait_for_target()

        @pl.when(jnp.logical_not(is_last))
        def _():
            for p in range(pieces):
                to_pair(own.at[p], p).wait_recv()
                own_on(p).start()

        to_pair(q_heads, pieces).wait_recv()

    lane = lax.broadcasted_iota(jnp.int32, (ROWS * line, PAD), 1)

    def arrives(step, p):
        landing(own, p, step, next_node, ring_send.at[0]).wait_recv()

    def chunk(step, carry):
        for p in range(pieces):
            arrives(step, p)

            @pl.when(step < steps - 2)
            def _():
                landing(ring.at[step], p, step + 1, next_node, ring_send.at[0]).start()

            @pl.when((step == steps - 2) & comes_last(p % heads))
            def _():
                landing(ring.at[step], p, step + 1, next_node, ring_send.at[1]).start()

            if p >= heads:
                attend(p - heads, ring[step, p - heads], ring[step, p])
        return carry

    lax.fori_loop(0, steps - 1, chunk, 0)

    def give(h):
        total = totals[h]
        high = total.astype(bf16)
        low = (total - high.astype(f32)).astype(bf16)
        parts_out[h] = jnp.where(lane >= HD + 16, low, high)
        for r, d, c in backs:
            if (r, d, c) != (0, 0, 0):
                give_back(r, d, c, h).start()

    for h in range(heads):

        @pl.when(jnp.logical_not(comes_last(h)))
        def _():
            give(h)

    for h in range(heads):

        @pl.when(comes_last(h))
        def _():
            arrives(steps - 1, h)
            arrives(steps - 1, heads + h)
            attend(h, ring[steps - 1, h], ring[steps - 1, heads + h])
            give(h)

    own_start = z_row * line + (x * 2 + core) * tokens
    for h in range(heads):
        parts_in[(core * ROWS + z_row) * COLUMNS + x, h] = parts_out[
            h, pl.ds(pl.multiple_of(own_start, tokens), tokens)
        ]

    def left(ref, sem):
        pltpu.make_async_copy(ref, ref, sem).wait()

    @pl.when(feeds_pair)
    def _():
        ways = COLUMNS - 1
        left(key_raw.at[0 : 2 * ways * tokens], feed_send.at[0])
        left(key_raw.at[0 : (ROWS * COLUMNS - 1) * tokens], feed_send.at[1])
        left(q_heads, pair_send.at[1])
        left(ring.at[0 : nodes - AHEAD - (1 if split else 2)], ring_send.at[0])
        left(ring.at[0, 0 : 2 * (heads - HEADS_UP) if split else pieces], ring_send.at[1])

        @pl.when(is_last)
        def _():
            left(own, ring_send.at[2])

        @pl.when(jnp.logical_not(is_last))
        def _():
            left(own, pair_send.at[0])

    @pl.when(core != FEED_CORE)
    def _():
        left(key_raw.at[0 : 2 * COLUMNS * tokens], feed_send.at[0])
        left(key_raw.at[0 : ROWS * COLUMNS * tokens], feed_send.at[1])
        left(ring.at[0, 0 : 2 * HEADS_UP], ring_send.at[1])

        @pl.when(is_last)
        def _():
            left(ring.at[0 : AHEAD - 2], ring_send.at[0])

        @pl.when(jnp.logical_not(is_last))
        def _():
            left(ring.at[0 : AHEAD - 1], ring_send.at[0])

    left(parts_out.at[:, 0 : (len(backs) - 1) * tokens], back_send)

    local_weight.wait()
    sent_weight.wait()
    attn = []
    others = parts_in.at[0 : len(backs) - 1]
    pltpu.make_async_copy(others, others, back_recv).wait()
    for d in range(COLUMNS):
        for h in range(heads):
            part = sum(
                parts_in[i * COLUMNS + d, h].astype(f32)
                for i in range(2 * ROWS)
            )
            total_weight = part[:, HD : HD + 1] + part[:, HD + 16 : HD + 17]
            attn.append((part[:, 0:HD] / total_weight).astype(bf16))
    attn = jnp.concatenate(attn, axis=1)
    mixed[...] = jnp.dot(attn, whole_weight[...], preferred_element_type=f32).astype(bf16)


def on_device(lines, query, key, value, q_gain, k_gain, out_weight):
    tokens, width = query.shape
    heads = width // HD // COLUMNS
    nodes = lines // ROWS
    pieces = 2 * heads
    most = max(AHEAD, nodes - AHEAD - (0 if HEADS_UP < heads else 1))
    line = 2 * COLUMNS * tokens
    window = 3 * PAD
    f32, bf16 = jnp.float32, jnp.bfloat16
    hbm = pl.BlockSpec(memory_space=pl.ANY)
    vmem = pl.BlockSpec(memory_space=pltpu.VMEM)
    dma = pltpu.SemaphoreType.DMA
    return pl.pallas_call(
        functools.partial(kernel, nodes, heads),
        out_shape=pltpu.VMEM((tokens, out_weight.shape[1]), bf16),
        in_specs=[hbm] * 6,
        out_specs=vmem,
        scratch_shapes=[
            pltpu.VMEM((3, tokens, width), bf16),
            pltpu.VMEM((line, window), bf16),
            pltpu.VMEM((line, window), bf16),
            pltpu.VMEM((ROWS, line, window), bf16),
            pltpu.VMEM((2, window, line), f32),
            pltpu.VMEM((2, 1, HD), f32),
            pltpu.VMEM((PAD, PAD), f32),
            pltpu.VMEM((pieces, HD, line), bf16),
            pltpu.VMEM((most, pieces, HD, line), bf16),
            pltpu.VMEM((heads, ROWS * line, PAD), bf16),
            pltpu.VMEM((heads, ROWS * line, PAD), f32),
            pltpu.VMEM((heads, ROWS * line, PAD), bf16),
            pltpu.VMEM((2 * ROWS * COLUMNS, heads, tokens, PAD), bf16),
            pltpu.VMEM((2 * out_weight.shape[0], out_weight.shape[1]), bf16),
            dma((3,)),
            dma((2,)),
            dma((2,)),
            dma((2 + ROWS,)),
            dma((3,)),
            dma((most, pieces)),
            dma,
            dma,
            dma((3,)),
            dma((2,)),
            dma((pieces + 1,)),
            pltpu.SemaphoreType.REGULAR,
            pltpu.SemaphoreType.REGULAR,
        ],
        compiler_params=pltpu.CompilerParams(collective_id=0, has_side_effects=True),
        name="attention",
    )(query, key, value, q_gain.reshape(1, HD), k_gain.reshape(1, HD), out_weight)


def solution(mesh):
    tokens = P(("grp", "blk", "uly"), None)
    return jax.shard_map(
        functools.partial(on_device, mesh.shape["blk"] // COLUMNS),
        mesh=mesh,
        in_specs=(tokens, tokens, tokens, P(), P(), P("uly", None)),
        out_specs=tokens,
        check_vma=False,
    )
```

```python
import functools
import math

import jax
import jax.numpy as jnp
from jax import lax
from jax.experimental import pallas as pl
from jax.experimental.pallas import tpu as pltpu
from jax.sharding import PartitionSpec as P

HD = 96
PAD = 128
COLUMNS = 4
ROWS = 2
FEED_CORE = 1
AHEAD = 6
HEADS_UP = 3
MESH = pl.DeviceIdType.MESH
TN = (((1,), (1,)), ((), ()))


def kernel(
    nodes,
    heads,
    query,
    key,
    value,
    q_gain,
    k_gain,
    weight,
    mixed,
    stage,
    key_raw,
    value_raw,
    query_raw,
    turned,
    gain_rows,
    gain_pad,
    own,
    ring,
    q_heads,
    totals,
    parts_out,
    parts_in,
    whole_weight,
    stage_sem,
    gain_sem,
    feed_send,
    feed_recv,
    ring_send,
    ring_recv,
    back_send,
    back_recv,
    weight_sem,
    pair_send,
    pair_recv,
    ready,
    row_ready,
):
    f32, bf16 = jnp.float32, jnp.bfloat16
    block = lax.axis_index("blk")
    core = lax.axis_index("uly")
    z, x = lax.div(block, COLUMNS), lax.rem(block, COLUMNS)
    z_block, z_row = lax.div(z, ROWS), lax.rem(z, ROWS)
    feeds_pair = core == FEED_CORE
    tokens = query.shape[0]
    window = 3 * PAD
    lanes = 2 * PAD
    group = heads * HD
    line = 2 * COLUMNS * tokens
    pieces = 2 * heads
    split = HEADS_UP < heads
    steps = jnp.where(feeds_pair, nodes - AHEAD - (0 if split else 1), AHEAD)

    def device(row, column, a_core):
        return {"blk": row * COLUMNS + column, "uly": a_core}

    def other_row(r):
        return z_block * ROWS + lax.rem(z_row + r, ROWS)

    def other_column(d):
        return lax.rem(x + d, COLUMNS)

    node, last_node = z_block, nodes - 1
    ahead = lax.rem(z + ROWS, nodes * ROWS)
    behind = lax.rem(z + last_node * ROWS, nodes * ROWS)
    is_first, is_last = node == 0, node == last_node

    staged = [
        pltpu.make_async_copy(src, stage.at[i], stage_sem.at[i])
        for i, src in enumerate((key, value, query))
    ]
    gains = [
        pltpu.make_async_copy(src, gain_rows.at[i], gain_sem.at[i])
        for i, src in enumerate((q_gain, k_gain))
    ]
    for copy in staged + gains:
        copy.start()

    barrier = pltpu.get_barrier_semaphore()

    def greet(dev):
        pl.semaphore_signal(barrier, inc=1, device_id=dev, device_id_type=MESH)

    first_row = z_row == 0

    @pl.when(feeds_pair)
    def _():
        for d in range(COLUMNS):
            for c in range(2):
                if (d, c) != (0, 0):
                    greet(device(z, other_column(d), lax.rem(core + c, 2)))

    @pl.when(first_row & (feeds_pair | (node != 0)))
    def _():
        for d in range(COLUMNS):
            greet(device(z + 1, other_column(d), FEED_CORE))

    @pl.when(first_row & feeds_pair)
    def _():
        for d in range(COLUMNS):
            greet(device(z + 1, other_column(d), 1 - FEED_CORE))

    before = jnp.where(
        feeds_pair,
        jnp.where(first_row, COLUMNS - 1, jnp.where(is_first, 2, 3) * COLUMNS - 1),
        jnp.where(first_row, COLUMNS, 2 * COLUMNS),
    )

    greets_ahead = jnp.where(feeds_pair, node != last_node, (node != 0) & (node != last_node))
    greets_behind = jnp.where(feeds_pair, node == 0, node < 2)
    lower = jnp.where(feeds_pair, node != 0, node != 1).astype(jnp.int32) + jnp.where(is_last, 1, 0)
    over_wrap = feeds_pair & is_last
    lower = lower + jnp.where(over_wrap, 1, 0)

    @pl.when(greets_ahead)
    def _():
        greet(device(ahead, x, core))

    @pl.when(greets_behind)
    def _():
        greet(device(behind, x, core))

    @pl.when(is_first & ~feeds_pair)
    def _():
        greet(device(behind, x, FEED_CORE))

    pl.semaphore_wait(barrier, before + lower)

    def tell(row, column, a_core, times):
        pl.semaphore_signal(
            row_ready, inc=times, device_id=device(row, column, a_core), device_id_type=MESH
        )

    for c in range(2):

        @pl.when(feeds_pair & ~first_row & ((node != 0) | (c == FEED_CORE)))
        def _():
            for d in range(COLUMNS):
                tell(z - 1, other_column(d), c, 1)

    target = jnp.where(feeds_pair, behind, ahead)
    source = jnp.where(feeds_pair, ahead, behind)

    @pl.when(jnp.where(feeds_pair, node == last_node, node > 1))
    def _():
        pl.semaphore_signal(ready, inc=1, device_id=device(source, x, core), device_id_type=MESH)

    def wait_for_target():
        @pl.when(jnp.where(feeds_pair, node == 0, (node != 0) & (node != last_node)))
        def _():
            pl.semaphore_wait(ready, 1)

    place = pl.ds(pl.multiple_of((x * 2 + core) * tokens, tokens), tokens)

    def feed(i, r, d):
        column = other_column(d)
        dst = (key_raw, value_raw, query_raw.at[z_row])[i].at[place]
        recv = feed_recv.at[i] if i < 2 else feed_recv.at[2 + z_row]
        return pltpu.make_async_remote_copy(
            src_ref=stage.at[i, :, pl.ds(pl.multiple_of(column * lanes, PAD), window)],
            dst_ref=dst,
            send_sem=feed_send.at[i // 2],
            recv_sem=recv,
            device_id=device(other_row(r), column, FEED_CORE),
            device_id_type=MESH,
        )

    def own_feed(i):
        dst = (key_raw, value_raw, query_raw.at[z_row])[i].at[place]
        recv = feed_recv.at[i] if i < 2 else feed_recv.at[2 + z_row]
        src = (key, value, query)[i]
        return pltpu.make_async_copy(
            src.at[:, pl.ds(pl.multiple_of(x * lanes, PAD), window)], dst, recv
        )

    feeds = [(i, r, d) for i in range(3) for r in range(ROWS if i == 2 else 1) for d in (2, 1, 3, 0)]
    for i, r, d in feeds:
        if (r, d) == (0, 2):
            staged[i].wait()
        if (r, d) == (1, 2):

            @pl.when(first_row)
            def _():
                pl.semaphore_wait(row_ready, COLUMNS)

        if (r, d) == (0, 0):

            @pl.when(feeds_pair)
            def _():
                own_feed(i).start()

            @pl.when(core != FEED_CORE)
            def _():
                feed(i, r, d).start()

        else:
            feed(i, r, d).start()

    depth = weight.shape[0]
    mine = whole_weight.at[pl.ds(pl.multiple_of(core * depth, 16), depth)]
    local_weight = pltpu.make_async_copy(weight, mine, weight_sem.at[0])
    sent_weight = pltpu.make_async_remote_copy(
        src_ref=weight,
        dst_ref=mine,
        send_sem=weight_sem.at[1],
        recv_sem=weight_sem.at[2],
        device_id=device(z, x, 1 - core),
        device_id_type=MESH,
    )
    local_weight.start()

    @pl.when(core != FEED_CORE)
    def _():
        sent_weight.start()

    def give_back(r, d, c, h):
        column, a_core = other_column(d), lax.rem(core + c, 2)
        row = lax.rem(z_row + r, ROWS)
        start = row * line + (column * 2 + a_core) * tokens
        return pltpu.make_async_remote_copy(
            src_ref=parts_out.at[h, pl.ds(pl.multiple_of(start, tokens), tokens)],
            dst_ref=parts_in.at[(core * ROWS + z_row) * COLUMNS + x, h],
            send_sem=back_send,
            recv_sem=back_recv,
            device_id=device(other_row(r), column, a_core),
            device_id_type=MESH,
        )

    backs = [(r, d, c) for r in (1, 0) for d in (2, 1, 3, 0) for c in range(2)]

    def landing(src, p, step, dev, send_sem):
        return pltpu.make_async_remote_copy(
            src_ref=src.at[p],
            dst_ref=ring.at[step, p],
            send_sem=send_sem,
            recv_sem=ring_recv.at[step, p],
            device_id=dev,
            device_id_type=MESH,
        )

    next_node = device(target, x, core)

    def own_on(p):
        return landing(own, p, 0, next_node, ring_send.at[0])

    def own_over_wrap(p):
        return landing(own, p, 0, device(ahead, x, 1 - core), ring_send.at[2])

    def comes_last(h):
        return feeds_pair | ~feeds_pair if not split else feeds_pair if h >= HEADS_UP else ~feeds_pair

    def to_pair(ref, p):
        return pltpu.make_async_remote_copy(
            src_ref=ref,
            dst_ref=ref,
            send_sem=pair_send.at[p // pieces],
            recv_sem=pair_recv.at[p],
            device_id=device(z, x, 1 - core),
            device_id_type=MESH,
        )

    scale = float(HD) ** (-0.5) * math.log2(math.e)

    def attend(h, k, v):
        k = jnp.concatenate([k, jnp.zeros((PAD - HD, line), bf16)], axis=0)
        v = jnp.concatenate([v, jnp.ones((PAD - HD, line), bf16)], axis=0)
        scores = jnp.dot(q_heads[h], k, preferred_element_type=f32)
        expd = jnp.exp2(scores * scale).astype(bf16)
        totals[h] += lax.dot_general(expd, v, TN, preferred_element_type=f32)

    totals[...] = jnp.zeros_like(totals)

    @pl.when(feeds_pair)
    def _():
        for i in range(2):
            gains[i].wait()
            gain_pad[...] = jnp.zeros_like(gain_pad)
            gain_pad[:, 0:HD] = jnp.broadcast_to(gain_rows[i], (PAD, HD))
            turned[i, 0:PAD, :] = gain_pad[...].T
        q_column, k_column = turned[0, 0:HD, :], turned[1, 0:HD, :]
        first = x * (group - lanes)

        def head_of(i, h):
            return turned[i, pl.ds(pl.multiple_of(first + h * HD, 32), HD), :]

        def normed(data, gain):
            meansq = jnp.mean(data * data, axis=0, keepdims=True)
            return data * lax.rsqrt(meansq + 1e-06) * gain

        def send_own(kind):
            mine = range(kind * heads, (kind + 1) * heads)

            @pl.when(is_last)
            def _():
                for p in mine:
                    own_over_wrap(p).start()

            @pl.when(node != 0)
            def _():
                for p in mine:
                    own_on(p).start()

            @pl.when(jnp.logical_not(is_last))
            def _():
                for p in mine:
                    to_pair(own.at[p], p).start()

        pltpu.make_async_copy(key_raw, key_raw, feed_recv.at[0]).wait()

        @pl.when(is_first & first_row)
        def _():
            tell(z, x, 1 - FEED_CORE, COLUMNS)

        turned[0] = key_raw[...].astype(f32).T
        for h in range(heads):
            own[h] = normed(head_of(0, h), k_column).astype(bf16)
        send_own(0)
        pltpu.make_async_copy(value_raw, value_raw, feed_recv.at[1]).wait()
        turned[1] = value_raw[...].astype(f32).T
        for h in range(heads):
            own[heads + h] = head_of(1, h).astype(bf16)
        send_own(1)

        for r in range(ROWS):
            rows = query_raw.at[r]
            pltpu.make_async_copy(rows, rows, feed_recv.at[2 + r]).wait()
            turned[0] = query_raw[r].astype(f32).T
            for h in range(heads):
                data = normed(head_of(0, h), q_column)
                data = jnp.concatenate([data, jnp.zeros((PAD - HD, line), f32)], axis=0)
                q_heads[h, r * line : (r + 1) * line, :] = data.T.astype(bf16)

        to_pair(q_heads, pieces).start()
        sent_weight.start()
        for h in range(heads):
            attend(h, own[h], own[heads + h])
        wait_for_target()

        @pl.when(node == 0)
        def _():
            for p in range(pieces):
                own_on(p).start()

    @pl.when(core != FEED_CORE)
    def _():
        for copy in gains:
            copy.wait()
        wait_for_target()

        @pl.when(jnp.logical_not(is_last))
        def _():
            for p in range(pieces):
                to_pair(own.at[p], p).wait_recv()
                own_on(p).start()

        to_pair(q_heads, pieces).wait_recv()

    lane = lax.broadcasted_iota(jnp.int32, (ROWS * line, PAD), 1)

    def arrives(step, p):
        landing(own, p, step, next_node, ring_send.at[0]).wait_recv()

    def chunk(step, carry):
        for p in range(pieces):
            arrives(step, p)

            @pl.when(step < steps - 2)
            def _():
                landing(ring.at[step], p, step + 1, next_node, ring_send.at[0]).start()

            @pl.when((step == steps - 2) & comes_last(p % heads))
            def _():
                landing(ring.at[step], p, step + 1, next_node, ring_send.at[1]).start()

            if p >= heads:
                attend(p - heads, ring[step, p - heads], ring[step, p])
        return carry

    lax.fori_loop(0, steps - 1, chunk, 0)

    def give(h):
        total = totals[h]
        high = total.astype(bf16)
        low = (total - high.astype(f32)).astype(bf16)
        parts_out[h] = jnp.where(lane >= HD + 16, low, high)
        for r, d, c in backs:
            if (r, d, c) != (0, 0, 0):
                give_back(r, d, c, h).start()

    for h in range(heads):

        @pl.when(jnp.logical_not(comes_last(h)))
        def _():
            give(h)

    for h in range(heads):

        @pl.when(comes_last(h))
        def _():
            arrives(steps - 1, h)
            arrives(steps - 1, heads + h)
            attend(h, ring[steps - 1, h], ring[steps - 1, heads + h])
            give(h)

    own_start = z_row * line + (x * 2 + core) * tokens
    for h in range(heads):
        parts_in[(core * ROWS + z_row) * COLUMNS + x, h] = parts_out[
            h, pl.ds(pl.multiple_of(own_start, tokens), tokens)
        ]

    def left(ref, sem):
        pltpu.make_async_copy(ref, ref, sem).wait()

    @pl.when(feeds_pair)
    def _():
        ways = COLUMNS - 1
        left(key_raw.at[0 : 2 * ways * tokens], feed_send.at[0])
        left(key_raw.at[0 : (ROWS * COLUMNS - 1) * tokens], feed_send.at[1])
        left(q_heads, pair_send.at[1])
        left(ring.at[0 : nodes - AHEAD - (1 if split else 2)], ring_send.at[0])
        left(ring.at[0, 0 : 2 * (heads - HEADS_UP) if split else pieces], ring_send.at[1])

        @pl.when(is_last)
        def _():
            left(own, ring_send.at[2])

        @pl.when(jnp.logical_not(is_last))
        def _():
            left(own, pair_send.at[0])

    @pl.when(core != FEED_CORE)
    def _():
        left(key_raw.at[0 : 2 * COLUMNS * tokens], feed_send.at[0])
        left(key_raw.at[0 : ROWS * COLUMNS * tokens], feed_send.at[1])
        left(ring.at[0, 0 : 2 * HEADS_UP], ring_send.at[1])

        @pl.when(is_last)
        def _():
            left(ring.at[0 : AHEAD - 2], ring_send.at[0])

        @pl.when(jnp.logical_not(is_last))
        def _():
            left(ring.at[0 : AHEAD - 1], ring_send.at[0])

    left(parts_out.at[:, 0 : (len(backs) - 1) * tokens], back_send)

    local_weight.wait()
    sent_weight.wait()
    attn = []
    others = parts_in.at[0 : len(backs) - 1]
    pltpu.make_async_copy(others, others, back_recv).wait()
    for d in range(COLUMNS):
        for h in range(heads):
            part = sum(
                parts_in[i * COLUMNS + d, h].astype(f32)
                for i in range(2 * ROWS)
            )
            total_weight = part[:, HD : HD + 1] + part[:, HD + 16 : HD + 17]
            attn.append((part[:, 0:HD] / total_weight).astype(bf16))
    attn = jnp.concatenate(attn, axis=1)
    mixed[...] = jnp.dot(attn, whole_weight[...], preferred_element_type=f32).astype(bf16)


def on_device(lines, query, key, value, q_gain, k_gain, out_weight):
    tokens, width = query.shape
    heads = width // HD // COLUMNS
    nodes = lines // ROWS
    pieces = 2 * heads
    most = max(AHEAD, nodes - AHEAD - (0 if HEADS_UP < heads else 1))
    line = 2 * COLUMNS * tokens
    window = 3 * PAD
    f32, bf16 = jnp.float32, jnp.bfloat16
    hbm = pl.BlockSpec(memory_space=pl.ANY)
    vmem = pl.BlockSpec(memory_space=pltpu.VMEM)
    dma = pltpu.SemaphoreType.DMA
    return pl.pallas_call(
        functools.partial(kernel, nodes, heads),
        out_shape=pltpu.VMEM((tokens, out_weight.shape[1]), bf16),
        in_specs=[hbm] * 6,
        out_specs=vmem,
        scratch_shapes=[
            pltpu.VMEM((3, tokens, width), bf16),
            pltpu.VMEM((line, window), bf16),
            pltpu.VMEM((line, window), bf16),
            pltpu.VMEM((ROWS, line, window), bf16),
            pltpu.VMEM((2, window, line), f32),
            pltpu.VMEM((2, 1, HD), f32),
            pltpu.VMEM((PAD, PAD), f32),
            pltpu.VMEM((pieces, HD, line), bf16),
            pltpu.VMEM((most, pieces, HD, line), bf16),
            pltpu.VMEM((heads, ROWS * line, PAD), bf16),
            pltpu.VMEM((heads, ROWS * line, PAD), f32),
            pltpu.VMEM((heads, ROWS * line, PAD), bf16),
            pltpu.VMEM((2 * ROWS * COLUMNS, heads, tokens, PAD), bf16),
            pltpu.VMEM((2 * out_weight.shape[0], out_weight.shape[1]), bf16),
            dma((3,)),
            dma((2,)),
            dma((2,)),
            dma((2 + ROWS,)),
            dma((3,)),
            dma((most, pieces)),
            dma,
            dma,
            dma((3,)),
            dma((2,)),
            dma((pieces + 1,)),
            pltpu.SemaphoreType.REGULAR,
            pltpu.SemaphoreType.REGULAR,
        ],
        compiler_params=pltpu.CompilerParams(collective_id=0, has_side_effects=True),
        name="attention",
    )(query, key, value, q_gain.reshape(1, HD), k_gain.reshape(1, HD), out_weight)


def solution(mesh):
    tokens = P(("grp", "blk", "uly"), None)
    return jax.shard_map(
        functools.partial(on_device, mesh.shape["blk"] // COLUMNS),
        mesh=mesh,
        in_specs=(tokens, tokens, tokens, P(), P(), P("uly", None)),
        out_specs=tokens,
        check_vma=False,
    )
```
